32 devices in a mesh: member: 2 (over x), gx: 8 (over z, y), gy: 2 (over core).
Axes of the slice: x: 2, y: 2, z: 4, core: 2. Of those that a mesh axis runs over, the one named last changes fastest.
Arguments:
- conc: float32 [66, 4, 64, 256], P(None, None, ('member', 'gx'), 'gy'), parts along dimension 2, may hold values from 0.001 to 30
- winds: float32 [2, 4, 64, 256], P(None, None, ('member', 'gx'), 'gy'), parts along dimension 2, may hold values from -0.9 to 0.9
- diffusivity: float32 [3, 64, 256], P(None, ('member', 'gx'), 'gy'), parts along dimension 1, may hold values from 0.1 to 10
- emission: float32 [66, 64, 256], P(None, ('member', 'gx'), 'gy'), parts along dimension 1, may hold values from 0.1 to 1
- photo_rate: float32 [66], replicated, may hold values from 0.05 to 1
Outputs:
- conc_next: float32 [66, 4, 64, 256], P(None, None, ('member', 'gx'), 'gy'), parts along dimension 2
The draws below stay inside these ranges and needn't reach their ends.
There are 2 independent parts, one for each index of `member`. The reference program is written for one: setup_inputs(seed, part) draws one part's arguments, and reference() takes and returns one part's arrays. A program takes and returns all parts, laid end to end along the dimension named above; an argument that names none is the same for every part. Nothing has to cross between parts.
All inputs are finite; a program needn't handle non-finite values.
Results may differ from the reference program's by a relative error of at most 0.00002.
Values sent between devices are 32-bit elements; how exact they have to be, the bound alone decides.
A program may use at most 64 MiB of HBM per device.

```python
import math
import jax
import jax.numpy as jnp
from jax import lax

SPEC = 66
LEV = 4
NX = 32
NY = 256


def draw_conc(key, part):
    base_key = jax.random.fold_in(key, 11)
    faint_key = jax.random.fold_in(key, 13)
    peak_key = jax.random.fold_in(key, 14)
    spike_key = jax.random.fold_in(key, 15)
    plume_key = jax.random.fold_in(key, 16)
    shape = (SPEC, LEV, NX, NY)
    rough = jnp.exp(jax.random.uniform(base_key, shape, jnp.float32, jnp.log(0.2), jnp.log(2.0)))
    faint = jnp.exp(jax.random.uniform(faint_key, shape, jnp.float32, jnp.log(0.001), jnp.log(0.01)))
    peak = jnp.exp(jax.random.uniform(peak_key, shape, jnp.float32, jnp.log(2.0), jnp.log(10.0)))
    share = 0.05
    spike = jax.random.uniform(spike_key, shape, jnp.float32) < share
    plumes = jnp.where(spike, peak, faint)
    order = jnp.arange(SPEC)
    plume_species = ((jax.random.uniform(plume_key, (SPEC,), jnp.float32) < 0.5) | (order == 1)) & (order > 0)
    ramp = 1.0 + 2.0 * jnp.arange(NX, dtype=jnp.float32) / NX
    values = jnp.where(plume_species[:, None, None, None], plumes, rough)
    values = values * ramp[None, None, :, None]
    return values.astype(jnp.float32)


def block_levels(own_key, shape, shards, low, largest):
    def one(dim, parts):
        steps = jax.random.uniform(jax.random.fold_in(jax.random.fold_in(own_key, 6), dim), (parts,), jnp.float32, low / len(shards), largest / len(shards))
        return jnp.repeat(jnp.exp(steps), shape[dim] // parts).reshape((-1,) + (1,) * (len(shape) - dim - 1))

    factor_of = one(*shards[0])
    for cut in shards[1:]:
        factor_of = factor_of * one(*cut)
    return factor_of


def setup_inputs(seed: int = 0, part: int = 0) -> dict:
    seeds = jax.random.split(jax.random.key(seed), 6)
    own_keys = jax.random.split(jax.random.fold_in(seeds[5], part), 6)
    conc = draw_conc(jax.random.fold_in(jax.random.fold_in(seeds[5], part), 71), part)
    winds = jnp.clip(jax.random.uniform(own_keys[1], (2, LEV, NX, NY), jnp.float32, -0.9, 0.9) * block_levels(own_keys[1], (2, LEV, NX, NY), ((2, 8), (3, 2)), -0.4, 0.0), -0.9, 0.9)
    diffusivity = jnp.clip(jnp.exp(math.log(10.0) - 4.6051702 * jax.random.uniform(own_keys[2], (LEV - 1, NX, NY), jnp.float32) ** block_levels(own_keys[2], (LEV - 1, NX, NY), ((1, 8), (2, 2)), -0.2, 0.2)), 0.1, 10.0)
    emission = jnp.clip(jnp.exp(math.log(1.0) - 2.3025851 * jax.random.uniform(own_keys[3], (SPEC, NX, NY), jnp.float32) ** block_levels(own_keys[3], (SPEC, NX, NY), ((1, 8), (2, 2)), -0.2, 0.2)), 0.1, 1.0)
    photo_rate = jnp.clip(jnp.exp(jax.random.uniform(seeds[4], (SPEC,), jnp.float32, math.log(0.05), math.log(1.0))), 0.05, 1.0)
    return dict(conc=conc, winds=winds, diffusivity=diffusivity, emission=emission, photo_rate=photo_rate)


BETAS = (1.0 / 3.0, 0.5, 1.0)


def flux_div(field, courant, axis):
    count = field.shape[axis] - 6

    def cut(arr, start):
        return lax.slice_in_dim(arr, start, start + count + 1, axis=axis)

    face = 0.5 * (cut(courant, 2) + cut(courant, 3))
    mean = (37.0 * (cut(field, 2) + cut(field, 3)) - 8.0 * (cut(field, 1) + cut(field, 4)) + (cut(field, 0) + cut(field, 5))) / 60.0
    spread = (10.0 * (cut(field, 3) - cut(field, 2)) - 5.0 * (cut(field, 4) - cut(field, 1)) + (cut(field, 5) - cut(field, 0))) / 60.0
    flux = face * mean - jnp.abs(face) * spread
    return lax.slice_in_dim(flux, 1, count + 1, axis=axis) - lax.slice_in_dim(flux, 0, count, axis=axis)


def advance(padded, wind_east, wind_north, start, beta):
    dx = flux_div(padded, wind_east, 2)
    inner_x = padded[:, :, 3:-3, :]
    partial_x = inner_x - beta * dx
    dy = flux_div(partial_x, wind_north, 3)
    return start + (partial_x[:, :, :, 3:-3] - inner_x[:, :, :, 3:-3]) - beta * dy


def vertical_mix(fixed, diffusivity, emission):
    levels = fixed.shape[1]
    zero = jnp.zeros_like(diffusivity[:1])
    lower = jnp.concatenate([zero, diffusivity], axis=0)
    upper = jnp.concatenate([diffusivity, zero], axis=0)
    diag = 1.0 + lower + upper
    right = fixed.at[:, 0].add(emission)
    ratio = [None] * levels
    value = [None] * levels
    ratio[0] = -upper[0] / diag[0]
    value[0] = right[:, 0] / diag[0]
    for lev in range(1, levels):
        pivot = diag[lev] + lower[lev] * ratio[lev - 1]
        ratio[lev] = -upper[lev] / pivot
        value[lev] = (right[:, lev] + lower[lev] * value[lev - 1]) / pivot
    result = [None] * levels
    result[levels - 1] = value[levels - 1]
    for lev in range(levels - 2, -1, -1):
        result[lev] = value[lev] - ratio[lev] * result[lev + 1]
    return jnp.stack(result, axis=1)


def photolysis(mixed, photo_rate):
    levels = mixed.shape[1]
    absorber = mixed[0]
    above = jnp.cumsum(absorber[::-1], axis=0)[::-1] - 0.5 * absorber
    column = above / levels
    rate = photo_rate[:, None, None, None] * jnp.exp(-0.5 * column)[None]
    return mixed * jnp.exp(-rate)


def reference(conc, winds, diffusivity, emission, photo_rate):
    margin = ((0, 0), (0, 0), (3, 3), (3, 3))
    padded_wind = jnp.pad(winds, margin)
    wind_east = padded_wind[0][None]
    wind_north = padded_wind[1][None][:, :, 3:-3, :]
    state = conc
    for beta in BETAS:
        state = advance(jnp.pad(state, margin), wind_east, wind_north, conc, beta)
    net = jnp.sum(state, axis=(1, 2, 3))
    positive = jnp.maximum(state, 0.0)
    total = jnp.sum(positive, axis=(1, 2, 3))
    fixed = positive * (net / total)[:, None, None, None]
    mixed = vertical_mix(fixed, diffusivity, emission)
    return photolysis(mixed, photo_rate)
```

```python
import functools

import jax
import jax.numpy as jnp
from jax import lax
from jax.experimental import pallas as pl
from jax.experimental.pallas import tpu as pltpu
from jax.sharding import PartitionSpec as P

BETAS = (1.0 / 3.0, 0.5, 1.0)
SUB = 8
LANES = 128
PAD = 3
CHUNKS = 3


def stencil_weights(km, kp):
    def face(k):
        k = k / 60.0
        a = jnp.abs(k)
        return (
            k + a,
            -8.0 * k - 5.0 * a,
            37.0 * k + 10.0 * a,
            37.0 * k - 10.0 * a,
            -8.0 * k + 5.0 * a,
            k - a,
        )

    m, p = face(km), face(kp)
    return [-m[0]] + [p[j] - m[j + 1] for j in range(5)] + [p[5]]


def kernel(dims, conc_hbm, wind_hbm, diff_hbm, emis_hbm, rate_ref, out_hbm,
           conc_ref, wind_ref, diff_ref, emis_ref,
           send, state0, state_a, state_b, result, back, wsend, wrecv, cbuf, wx, wy,
           stat, stats, prate, coef,
           load_sem, in_send, in_recv, w_send, w_recv, h_send, h_recv,
           out_send, out_recv, s_send, s_recv, out_ref, store_sem):
    spec, lev, rows, halves, gx_n, span, tiles, chunks = dims
    n = gx_n * halves
    width = tiles // chunks
    deep = span * rows
    crews = gx_n // span
    my_gx, my_gy = lax.axis_index("gx"), lax.axis_index("gy")
    me = my_gx * halves + my_gy
    crew, seat = my_gx // span, my_gx % span
    my_lev = seat * halves + my_gy
    has_down, has_up = crew > 0, crew < crews - 1

    def where_is(dev):
        return {"gx": dev // halves, "gy": dev % halves}

    barrier = pltpu.get_barrier_semaphore()

    def greet(k, carry):
        pl.semaphore_signal(barrier, inc=1, device_id=where_is((me + k) % n),
                            device_id_type=pl.DeviceIdType.MESH)
        return carry

    lax.fori_loop(1, n, greet, 0)
    loads = [pltpu.make_async_copy(src, dst, load_sem.at[i]) for i, (src, dst) in enumerate(
        ((wind_hbm, wind_ref), (conc_hbm, conc_ref), (diff_hbm, diff_ref), (emis_hbm, emis_ref)))]
    for load in loads:
        load.start()

    stride = lev * rows
    loads[0].wait()
    for lv in range(lev):
        wsend[lv, 0:rows, :] = wind_ref[pl.ds(lv * rows, rows), :]
        wsend[lv, rows:2 * rows, :] = wind_ref[pl.ds((lev + lv) * rows, rows), :]
    loads[1].wait()
    for t in range(tiles):
        have = max(0, min(SUB, spec - t * SUB))
        for lv in range(lev):
            for r in range(rows):
                if have < SUB:
                    send[lv, t, r, :, :] = jnp.zeros((SUB, LANES), jnp.float32)
                if have > 0:
                    send[lv, t, r, 0:have, :] = conc_ref[
                        pl.ds(t * SUB * stride + lv * rows + r, have, stride=stride), :]

    pl.semaphore_wait(barrier, n - 1)

    def remote(src, dst, dev, s_sem, r_sem):
        return pltpu.make_async_remote_copy(
            src_ref=src, dst_ref=dst, send_sem=s_sem, recv_sem=r_sem,
            device_id=where_is(dev), device_id_type=pl.DeviceIdType.MESH)

    def deliver(src, dst, dev, s_sem, r_sem):
        @pl.when(dev == me)
        def _():
            pltpu.make_async_copy(src, dst, r_sem).start()

        @pl.when(dev != me)
        def _():
            remote(src, dst, dev, s_sem, r_sem).start()

    def sent(src, s_sem):
        pltpu.make_async_copy(src, src, s_sem).wait()

    def landed(dst, r_sem):
        pltpu.make_async_copy(dst, dst, r_sem).wait()

    def mate(lv):
        return (crew * span + lv // halves) * halves + lv % halves

    def tile_range(c):
        return pl.ds(c * width, width)

    sides = ((0, None, None), (1, has_up & (seat == span - 1), 0),
             (-1, has_down & (seat == 0), span + 1))

    def for_winds(act):
        for o, (shift, cond, slot) in enumerate(sides):
            at = seat + 1 if slot is None else slot
            for lv in range(lev):
                dev = mate(lv) + shift * span * halves
                if cond is None:
                    act(o, lv, dev, at)
                else:
                    pl.when(cond)(functools.partial(act, o, lv, dev, at))

    for_winds(lambda o, lv, dev, at: deliver(
        wsend.at[lv], wrecv.at[at * halves + my_gy], dev, w_send.at[o, lv],
        w_recv.at[at * halves + my_gy]))
    for c in range(chunks):
        for lv in range(lev):
            deliver(send.at[lv, tile_range(c)],
                    state0.at[tile_range(c), my_gy, pl.ds(PAD + seat * rows, rows)],
                    mate(lv), in_send.at[lv, c], in_recv.at[my_lev, c])

    lane = lax.broadcasted_iota(jnp.int32, (SUB, LANES), 1)
    states = (state0, state_a, state_b)
    blank = jnp.zeros((PAD, SUB, LANES), jnp.float32)

    @pl.when(crew == 0)
    def _():
        for buf in states:
            for t in range(tiles):
                for h in range(halves):
                    buf[t, h, 0:PAD] = blank

    @pl.when(crew == crews - 1)
    def _():
        for buf in states:
            for t in range(tiles):
                for h in range(halves):
                    buf[t, h, PAD + deep:2 * PAD + deep] = blank

    for h in range(halves):
        for c in range(2):
            cbuf[c, h, 0:SUB, :] = jnp.zeros((SUB, LANES), jnp.float32)
            cbuf[c, h, SUB + deep:2 * SUB + deep, :] = jnp.zeros((SUB, LANES), jnp.float32)

    def wind_in(slot):
        for h in range(halves):
            landed(wrecv.at[slot * halves + h], w_recv.at[slot * halves + h])
            for c in range(2):
                base = SUB + (slot - 1) * rows
                cbuf[c, h, base:base + rows, :] = wrecv[
                    slot * halves + h, c * rows:(c + 1) * rows, :]

    for slot in range(1, span + 1):
        wind_in(slot)
    pl.when(has_down)(lambda: wind_in(0))
    pl.when(has_up)(lambda: wind_in(span + 1))
    for x0 in range(0, deep, SUB):
        for h in range(halves):
            here = cbuf[0, h, SUB + x0:SUB + x0 + SUB, :]
            left = cbuf[0, h, SUB + x0 - 1:SUB + x0 - 1 + SUB, :]
            right = cbuf[0, h, SUB + x0 + 1:SUB + x0 + 1 + SUB, :]
            for j, w in enumerate(stencil_weights(0.5 * (left + here), 0.5 * (here + right))):
                wx[j, h, x0:x0 + SUB, :] = w
        cy = [cbuf[1, h, SUB + x0:SUB + x0 + SUB, :] for h in range(halves)]
        zer = jnp.zeros((SUB, LANES), jnp.float32)
        for h in range(halves):
            nxt = pltpu.roll(cy[h + 1], LANES - 1, 1) if h + 1 < halves else zer
            prv = pltpu.roll(cy[h - 1], 1, 1) if h > 0 else zer
            up = jnp.where(lane < LANES - 1, pltpu.roll(cy[h], LANES - 1, 1), nxt)
            down = jnp.where(lane >= 1, pltpu.roll(cy[h], 1, 1), prv)
            ws = stencil_weights(0.5 * (down + cy[h]), 0.5 * (cy[h] + up))
            for j, w in enumerate(ws):
                d = j - 3
                if d > 0 and h == halves - 1:
                    w = jnp.where(lane < LANES - d, w, 0.0)
                if d < 0 and h == 0:
                    w = jnp.where(lane >= -d, w, 0.0)
                wy[j, h, x0:x0 + SUB, :] = w

    def halo(s, c, d):
        buf, own = states[s], tile_range(c)
        first, land = (deep, 0) if d == 0 else (PAD, PAD + deep)
        return remote(
            buf.at[own, :, pl.ds(first, PAD)], buf.at[own, :, pl.ds(land, PAD)],
            me + (span * halves if d == 0 else -span * halves),
            h_send.at[s, c, d], h_recv.at[s, c, d])

    def start_halo(s, c):
        pl.when(has_up)(lambda: halo(s, c, 0).start())
        pl.when(has_down)(lambda: halo(s, c, 1).start())

    def wait_halo(s, c):
        own = tile_range(c)
        pl.when(has_down)(lambda: landed(states[s].at[own, :, pl.ds(0, PAD)], h_recv.at[s, c, 0]))
        pl.when(has_up)(lambda: landed(
            states[s].at[own, :, pl.ds(PAD + deep, PAD)], h_recv.at[s, c, 1]))

    for c in range(chunks):
        for lv in range(lev):
            landed(state0.at[tile_range(c), lv % halves, pl.ds(PAD + (lv // halves) * rows, rows)],
                   in_recv.at[lv, c])
        start_halo(0, c)

    def stage(c, src, dst, off, beta, x, sums):
        wxs = [[wx[j, h, pl.ds(x, 1), :] * beta for j in range(7)] for h in range(halves)]
        wys = [[wy[j, h, pl.ds(x, 1), :] * beta for j in range(7)] for h in range(halves)]
        out = []
        for i in range(width):
            t = c * width + i
            partial, new = [], []
            for h in range(halves):
                acc = wxs[h][0] * src[t, h, x]
                for j in range(1, 7):
                    acc = acc + wxs[h][j] * src[t, h, x + j]
                mid = src[t, h, x + PAD]
                p = mid - acc
                partial.append(p)
                start = mid if src is state0 else state0[t, h, x + PAD]
                new.append(start - acc - wys[h][3] * p)
            for d in (1, 2, 3):
                up = [pltpu.roll(p, LANES - d, 1) for p in partial]
                down = [pltpu.roll(p, d, 1) for p in partial]
                for h in range(halves):
                    u = up[h] if h == halves - 1 else jnp.where(lane < LANES - d, up[h], up[h + 1])
                    w = down[h] if h == 0 else jnp.where(lane >= d, down[h], down[h - 1])
                    new[h] = new[h] - (wys[h][3 + d] * u + wys[h][3 - d] * w)
            for h in range(halves):
                dst[t, h, x + off] = new[h]
            if sums is not None:
                net, pos = sums[2 * i], sums[2 * i + 1]
                for v in new:
                    net, pos = net + v, pos + jnp.maximum(v, 0.0)
                out += [net, pos]
        return tuple(out)

    stat[...] = jnp.zeros((SUB, LANES), jnp.float32)
    for s in range(3):
        for c in range(chunks):
            wait_halo(s, c)
            if s < 2:

                @pl.loop(0, deep)
                def _(x):
                    stage(c, states[s], states[s + 1], PAD, BETAS[s], x, None)

                start_halo(s + 1, c)
                continue
            z = jnp.zeros((SUB, LANES), jnp.float32)
            sums = lax.fori_loop(
                0, deep, lambda x, v: stage(c, states[s], result, 0, BETAS[s], x, v),
                (z,) * (2 * width))
            for lv in range(lev):
                deliver(result.at[tile_range(c), lv % halves, pl.ds((lv // halves) * rows, rows)],
                        back.at[my_lev, tile_range(c)], mate(lv),
                        out_send.at[lv, c], out_recv.at[my_lev, c])
            acc = stat[...]
            for i in range(width):
                t = c * width + i
                net = jnp.sum(sums[2 * i], axis=1, keepdims=True)
                pos = jnp.sum(sums[2 * i + 1], axis=1, keepdims=True)
                acc = jnp.where(lane == t, net, jnp.where(lane == tiles + t, pos, acc))
            stat[...] = acc

    def send_stat(k, carry):
        dev = (k + me) % n
        deliver(stat, stats.at[me], dev, s_send.at[dev], s_recv.at[me])
        return carry

    lax.fori_loop(0, n, send_stat, 0)

    sub = lax.broadcasted_iota(jnp.int32, (SUB, LANES), 0)
    for t in range(tiles):
        tile = jnp.zeros((SUB, LANES), jnp.float32)
        for i in range(SUB):
            if t * SUB + i < spec:
                tile = jnp.where(sub == i, rate_ref[t * SUB + i], tile)
        prate[pl.ds(t * SUB, SUB), :] = tile
    loads[2].wait()
    loads[3].wait()
    ks = [diff_ref[lv] for lv in range(lev - 1)]
    zero = jnp.zeros((rows, LANES), jnp.float32)
    lower = [zero] + ks
    upper = ks + [zero]
    prev = None
    for lv in range(lev):
        pivot = 1.0 + lower[lv] + upper[lv]
        if lv:
            pivot = pivot + lower[lv] * prev
        inv = 1.0 / pivot
        prev = -upper[lv] * inv
        coef[0, pl.ds(lv * rows, rows), :] = inv
        coef[1, pl.ds(lv * rows, rows), :] = lower[lv]
        coef[2, pl.ds(lv * rows, rows), :] = -prev

    def stat_in(k, carry):
        landed(stats.at[k], s_recv.at[k])
        return carry

    for c in range(chunks):
        for lv in range(lev):
            landed(back.at[lv, tile_range(c)], out_recv.at[lv, c])
    lax.fori_loop(0, n, stat_in, 0)
    total = stats[0]
    for k in range(1, n):
        total = total + stats[k]

    fades = [None] * rows
    stores = []
    for t in range(tiles):
        have = min(SUB, spec - t * SUB)
        if have <= 0:
            continue
        scale = jnp.broadcast_to(
            total[:, t:t + 1] / total[:, tiles + t:tiles + t + 1], (SUB, LANES))
        rate = prate[pl.ds(t * SUB, SUB), :]
        for r in range(rows):
            emis = emis_ref[pl.ds(t * SUB * rows + r, have, stride=rows), :]
            if have < SUB:
                emis = jnp.concatenate(
                    [emis, jnp.zeros((SUB - have, LANES), jnp.float32)], axis=0)
            value = []
            for lv in range(lev):
                right = jnp.maximum(back[lv, t, r], 0.0) * scale
                if lv == 0:
                    right = right + emis
                else:
                    right = right + coef[1, pl.ds(lv * rows + r, 1), :] * value[-1]
                value.append(right * coef[0, pl.ds(lv * rows + r, 1), :])
            mixed = [None] * lev
            mixed[lev - 1] = value[lev - 1]
            for lv in range(lev - 2, -1, -1):
                mixed[lv] = value[lv] + coef[2, pl.ds(lv * rows + r, 1), :] * mixed[lv + 1]
            if t == 0:
                fade = [None] * lev
                above = jnp.zeros((1, LANES), jnp.float32)
                for lv in range(lev - 1, -1, -1):
                    mine = mixed[lv][0:1, :]
                    fade[lv] = jnp.exp((-0.5 / lev) * (above + 0.5 * mine))
                    above = above + mine
                fades[r] = fade
            for lv in range(lev):
                val = mixed[lv] * jnp.exp(-(rate * fades[r][lv]))
                out_hbm[pl.ds(t * SUB * stride + lv * rows + r, have, stride=stride), :] = val[0:have]
        done = pl.ds(t * SUB * stride, have * stride)

    def wind_sent(o, lv, dev, at):
        pl.when(dev != me)(lambda: sent(wsend.at[lv], w_send.at[o, lv]))

    for_winds(wind_sent)
    for lv in range(lev):

        @pl.when(lv != my_lev)
        def _():
            for c in range(chunks):
                sent(send.at[lv, tile_range(c)], in_send.at[lv, c])
                sent(result.at[tile_range(c), lv % halves, pl.ds((lv // halves) * rows, rows)],
                     out_send.at[lv, c])

    for s in range(3):
        for c in range(chunks):
            own = tile_range(c)
            pl.when(has_up)(lambda: sent(states[s].at[own, :, pl.ds(deep, PAD)], h_send.at[s, c, 0]))
            pl.when(has_down)(lambda: sent(states[s].at[own, :, pl.ds(PAD, PAD)], h_send.at[s, c, 1]))

    def stat_sent(k, carry):
        sent(stat, s_send.at[(k + me) % n])
        return carry

    lax.fori_loop(1, n, stat_sent, 0)


def per_device(gx_n, halves, conc, winds, diffusivity, emission, photo_rate):
    spec, lev, rows, lanes = conc.shape
    span = lev // halves
    assert span * halves == lev and gx_n % span == 0
    n = gx_n * halves
    real = -(-spec // SUB)
    chunks = CHUNKS
    width = -(-real // chunks)
    tiles = chunks * width
    deep = span * rows
    dims = (spec, lev, rows, halves, gx_n, span, tiles, chunks)
    f32 = jnp.float32
    hbm = pl.BlockSpec(memory_space=pl.ANY)
    dma = pltpu.SemaphoreType.DMA
    slots = (span + 2) * halves
    out = pl.pallas_call(
        functools.partial(kernel, dims),
        out_shape=pltpu.VMEM((spec * lev * rows, lanes), f32),
        in_specs=[hbm] * 4 + [pl.BlockSpec(memory_space=pltpu.SMEM)],
        out_specs=pl.BlockSpec(memory_space=pltpu.VMEM),
        scratch_shapes=[
            pltpu.VMEM((spec * lev * rows, lanes), f32),
            pltpu.VMEM((2 * lev * rows, lanes), f32),
            pltpu.VMEM((lev - 1, rows, lanes), f32),
            pltpu.VMEM((spec * rows, lanes), f32),
            pltpu.VMEM((lev, tiles, rows, SUB, lanes), f32),
            pltpu.VMEM((tiles, halves, deep + 2 * PAD, SUB, lanes), f32),
            pltpu.VMEM((tiles, halves, deep + 2 * PAD, SUB, lanes), f32),
            pltpu.VMEM((tiles, halves, deep + 2 * PAD, SUB, lanes), f32),
            pltpu.VMEM((tiles, halves, deep, SUB, lanes), f32),
            pltpu.VMEM((lev, tiles, rows, SUB, lanes), f32),
            pltpu.VMEM((lev, 2 * rows, lanes), f32),
            pltpu.VMEM((slots, 2 * rows, lanes), f32),
            pltpu.VMEM((2, halves, deep + 2 * SUB, lanes), f32),
            pltpu.VMEM((7, halves, deep, lanes), f32),
            pltpu.VMEM((7, halves, deep, lanes), f32),
            pltpu.VMEM((SUB, lanes), f32),
            pltpu.VMEM((n, SUB, lanes), f32),
            pltpu.VMEM((tiles * SUB, lanes), f32),
            pltpu.VMEM((3, lev * rows, lanes), f32),
            dma((4,)),
            dma((lev, chunks)), dma((lev, chunks)),
            dma((3, lev)), dma((slots,)),
            dma((3, chunks, 2)), dma((3, chunks, 2)),
            dma((lev, chunks)), dma((lev, chunks)),
            dma((n,)), dma((n,)),
            pltpu.VMEM((spec * lev * rows, lanes), f32), dma((tiles,)),
        ],
        compiler_params=pltpu.CompilerParams(collective_id=0, has_side_effects=True),
    )(
        conc.reshape(spec * lev * rows, lanes),
        winds.reshape(2 * lev * rows, lanes),
        diffusivity,
        emission.reshape(spec * rows, lanes),
        photo_rate,
    )
    return out.reshape(spec, lev, rows, lanes)


def solution(mesh):
    halves = mesh.shape["gy"]
    gx_n = mesh.shape["gx"]
    return jax.shard_map(
        functools.partial(per_device, gx_n, halves),
        mesh=mesh,
        in_specs=(
            P(None, None, ("member", "gx"), "gy"),
            P(None, None, ("member", "gx"), "gy"),
            P(None, ("member", "gx"), "gy"),
            P(None, ("member", "gx"), "gy"),
            P(),
        ),
        out_specs=P(None, None, ("member", "gx"), "gy"),
        check_vma=False,
    )
```

```python
import functools

import jax
import jax.numpy as jnp
from jax import lax
from jax.experimental import pallas as pl
from jax.experimental.pallas import tpu as pltpu
from jax.sharding import PartitionSpec as P

BETAS = (1.0 / 3.0, 0.5, 1.0)
SUB = 8
LANES = 128
PAD = 3
WIDE = 2 * PAD
AHEAD = 11
LAG_A = 4
LAG_B = 8
LAG_U = 12
MESH = pl.DeviceIdType.MESH


def stencil_weights(km, kp):
    def face(k):
        k = k / 60.0
        a = jnp.abs(k)
        return (
            k + a,
            -8.0 * k - 5.0 * a,
            37.0 * k + 10.0 * a,
            37.0 * k - 10.0 * a,
            -8.0 * k + 5.0 * a,
            k - a,
        )

    m, p = face(km), face(kp)
    return [-m[0]] + [p[j] - m[j + 1] for j in range(5)] + [p[5]]


def kernel(dims, conc_hbm, wind_hbm, diff_hbm, emis_hbm, rate_ref, out_ref,
           diff_ref, emis_ref, state0, state1, state2, result, back,
           wrecv, cbuf, wts, part, stat, stats, scal,
           load_sem, w_send, w_recv, in_send, in_recv, d_send, r_send, a_recv,
           b_send, b_recv, out_send, out_recv, s_send, s_recv):
    spec, lev, rows, halves, gx_n, span, chunk = dims
    n = gx_n * halves
    chunks = spec // chunk
    deep = span * rows
    crews = gx_n // span
    slab, slab1, slab2 = deep + 2 * SUB, 2 * SUB, 2 * SUB
    my_gx, my_gy = lax.axis_index("gx"), lax.axis_index("gy")
    me = my_gx * halves + my_gy
    crew, seat = my_gx // span, my_gx % span
    my_lev = seat * halves + my_gy
    has_down, has_up = crew > 0, crew < crews - 1
    shift = span * halves

    def where_is(dev):
        return {"gx": dev // halves, "gy": dev % halves}

    def mate(at, half):
        return (crew * span + at) * halves + half

    barrier = pltpu.get_barrier_semaphore()

    def greet(k, carry):
        pl.semaphore_signal(barrier, inc=1, device_id=where_is((me + k) % n), device_id_type=MESH)
        return carry

    lax.fori_loop(1, n, greet, 0)
    loads = [pltpu.make_async_copy(src, dst, load_sem.at[i]) for i, (src, dst) in enumerate(
        ((diff_hbm, diff_ref), (emis_hbm, emis_ref)))]
    for load in loads:
        load.start()

    def push(src, dst, dev, s_sem, r_sem):
        pltpu.make_async_remote_copy(
            src_ref=src, dst_ref=dst, send_sem=s_sem, recv_sem=r_sem,
            device_id=where_is(dev), device_id_type=MESH).start()

    def local(src, dst, r_sem):
        pltpu.make_async_copy(src, dst, r_sem).start()

    def take(like, sem):
        pltpu.make_async_copy(like, like, sem).wait()

    def group(c):
        return pl.ds(c * chunk, chunk)

    flat0 = state0.reshape(halves * spec * slab, LANES)
    flat1 = state1.reshape(halves * chunk * slab1, LANES)
    flat2 = state2.reshape(halves * spec * slab2, LANES)
    flat_r = result.reshape(halves * spec * deep, LANES)
    flat_b = back.reshape(spec * lev * rows, LANES)
    zero = jnp.zeros((SUB, LANES), jnp.float32)
    few = jnp.zeros((SUB // 2, LANES), jnp.float32)

    def clear(first0, first2):
        @pl.loop(0, halves * spec)
        def _(i):
            flat0[pl.ds(i * slab + first0, SUB), :] = zero
            flat2[pl.ds(i * slab2 + first2, SUB // 2), :] = few

    pl.when(crew == 0)(lambda: clear(0, 0))
    pl.when(crew == crews - 1)(lambda: clear(SUB + deep, SUB // 2 + deep))
    for h in range(halves):
        for c in range(2):
            cbuf[c, h, 0:SUB, :] = zero
            cbuf[c, h, SUB + deep:2 * SUB + deep, :] = zero
    part[...] = jnp.zeros_like(part)
    stat[...] = zero

    pl.semaphore_wait(barrier, n - 1)

    own_rows = pl.ds(SUB + seat * rows, rows)

    def send_in(c):
        dst = state0.at[my_gy, group(c), own_rows]
        for k in range(1, span):
            at = (seat + k) % span
            for h in range(halves):
                push(conc_hbm.at[group(c), at * halves + h], dst, mate(at, h),
                     in_send.at[k * halves + h], in_recv.at[seat, c])
        for k in range(1, halves):
            h = (my_gy + k) % halves
            push(conc_hbm.at[group(c), seat * halves + h], dst, mate(seat, h),
                 in_send.at[k], in_recv.at[seat, c])
        local(conc_hbm.at[group(c), my_lev], dst, in_recv.at[seat, c])

    def reach(at, up):
        if up:
            first = max(0, deep - WIDE - at * rows)
            return first, rows - first, SUB - deep + at * rows + first
        return 0, max(0, min(rows, WIDE - at * rows)), SUB + deep + at * rows

    def each_way(act):
        for up, cond in ((1, has_up), (0, has_down)):
            for at in range(span):
                pl.when(cond & (seat == at))(functools.partial(act, up, at))

    def send_direct(c):
        def act(up, at):
            first, count, land = reach(at, up)
            if count > 0:
                for h in range(halves):
                    push(conc_hbm.at[group(c), at * halves + h, pl.ds(first, count)],
                         state0.at[my_gy, group(c), pl.ds(land, count)],
                         mate(at, h) + (shift if up else -shift),
                         d_send.at[up, h], a_recv.at[up, c])

        each_way(act)

    def send_relay(c):
        def act(up, at):
            for other in range(span):
                first, count, land = reach(other, up)
                if other != at and count > 0:
                    push(state0.at[:, group(c), pl.ds(SUB + other * rows + first, count)],
                         state0.at[:, group(c), pl.ds(land, count)],
                         me + (shift if up else -shift), r_send.at[up], a_recv.at[up, c])

        each_way(act)

    sides = ((0, None, None), (1, has_up & (seat == span - 1), 0),
             (-1, has_down & (seat == 0), span + 1))

    def for_winds(act):
        for o, (step, cond, slot) in enumerate(sides):
            at = seat + 1 if slot is None else slot
            for lv in range(lev):
                dev = mate(lv // halves, lv % halves) + step * shift
                if cond is None:
                    pl.when(dev != me)(functools.partial(act, o, lv, dev, at))
                else:
                    pl.when(cond)(functools.partial(act, o, lv, dev, at))

    for_winds(lambda o, lv, dev, at: push(
        wind_hbm.at[:, lv], wrecv.at[at * halves + my_gy], dev, w_send.at[o, lv],
        w_recv.at[at * halves + my_gy]))
    local(wind_hbm.at[:, my_lev], wrecv.at[(seat + 1) * halves + my_gy],
          w_recv.at[(seat + 1) * halves + my_gy])

    @pl.loop(0, chunks)
    def _(c):
        send_in(c)
        pl.when(c < AHEAD)(lambda: send_direct(c))

    lane = lax.broadcasted_iota(jnp.int32, (SUB, LANES), 1)
    sub = lax.broadcasted_iota(jnp.int32, (SUB, LANES), 0)

    for load in loads:
        load.wait()
    ks = [diff_ref[lv] for lv in range(lev - 1)]
    none = jnp.zeros((rows, LANES), jnp.float32)
    lower, upper = [none] + ks, ks + [none]
    inv, ratio = [], []
    for lv in range(lev):
        pivot = 1.0 + lower[lv] + upper[lv]
        if lv:
            pivot = pivot - lower[lv] * ratio[-1]
        inv.append(1.0 / pivot)
        ratio.append(upper[lv] * inv[lv])
    inverse = [[None] * lev for _ in range(lev)]
    for j in range(lev):
        val = [none] * lev
        for lv in range(j, lev):
            val[lv] = inv[lv] if lv == j else lower[lv] * val[lv - 1] * inv[lv]
        for lv in range(lev - 1, -1, -1):
            inverse[lv][j] = val[lv] if lv == lev - 1 else val[lv] + ratio[lv] * inverse[lv + 1][j]
    pairs = lev // 2

    def duo(a, b):
        return jnp.concatenate([a, b], axis=0)

    mats = [[(duo(inverse[2 * o][2 * i], inverse[2 * o + 1][2 * i + 1]),
              duo(inverse[2 * o][2 * i + 1], inverse[2 * o + 1][2 * i]))
             for i in range(pairs)] for o in range(pairs)]
    first_col = [duo(inverse[2 * o][0], inverse[2 * o + 1][0]) for o in range(pairs)]

    def flip(v):
        return pltpu.roll(v, SUB // 2, 0)

    low = sub < SUB // 2

    @pl.loop(0, spec // 2)
    def _(s):
        e = emis_ref[pl.ds(s * SUB, SUB), :]
        f = flip(e)
        for k, v in enumerate((jnp.where(low, e, f), jnp.where(low, f, e))):
            for o in range(pairs):
                out_ref[pl.ds((2 * s + k) * lev * rows + o * SUB, SUB), :] = first_col[o] * v

    def wind_in(slot):
        for h in range(halves):
            take(wrecv.at[slot * halves + h], w_recv.at[slot * halves + h])
            for c in range(2):
                base = SUB + (slot - 1) * rows
                cbuf[c, h, base:base + rows, :] = wrecv[slot * halves + h, c]

    for slot in range(1, span + 1):
        wind_in(slot)
    pl.when(has_down)(lambda: wind_in(0))
    pl.when(has_up)(lambda: wind_in(span + 1))

    passes = ((0, -PAD), (0, deep - SUB + PAD), (1, 0), (2, 0))
    for q, (s, r0) in enumerate(passes):
        at_row = crew * deep + r0 + sub
        inside = (at_row >= 0) & (at_row < crews * deep)
        for h in range(halves):
            here, left, right = (cbuf[0, h, SUB + r0 + d:2 * SUB + r0 + d, :] for d in (0, -1, 1))
            for j, w in enumerate(stencil_weights(0.5 * (left + here), 0.5 * (here + right))):
                wts[q, h, j] = jnp.where(inside, w, 0.0) * BETAS[s]
        cy = [cbuf[1, h, SUB + r0:2 * SUB + r0, :] for h in range(halves)]
        for h in range(halves):
            nxt = pltpu.roll(cy[h + 1], LANES - 1, 1) if h + 1 < halves else zero
            prv = pltpu.roll(cy[h - 1], 1, 1) if h > 0 else zero
            up = jnp.where(lane < LANES - 1, pltpu.roll(cy[h], LANES - 1, 1), nxt)
            down = jnp.where(lane >= 1, pltpu.roll(cy[h], 1, 1), prv)
            ws = stencil_weights(0.5 * (down + cy[h]), 0.5 * (cy[h] + up))
            for j, w in enumerate(ws):
                d = j - 3
                if d > 0 and h == halves - 1:
                    w = jnp.where(lane < LANES - d, w, 0.0)
                if d < 0 and h == 0:
                    w = jnp.where(lane >= -d, w, 0.0)
                wts[q, h, 7 + j] = w * BETAS[s]

    def step(q, count, src, src_at, start, start_at, put):
        wx = [[wts[q, h, j] for j in range(7)] for h in range(halves)]
        wy = [[wts[q, h, 7 + j] for j in range(7)] for h in range(halves)]
        for i in range(count):
            partial, new = [], []
            for h in range(halves):
                base = src_at(h, i)
                mid = None
                acc = None
                for j in range(7):
                    v = src[pl.ds(base + j, SUB), :]
                    if j == PAD:
                        mid = v
                    acc = wx[h][j] * v if acc is None else acc + wx[h][j] * v
                p = mid - acc
                partial.append(p)
                begin = mid if start is None else start[pl.ds(start_at(h, i), SUB), :]
                new.append(begin - acc - wy[h][3] * p)
            for d in (1, 2, 3):
                up = [pltpu.roll(p, LANES - d, 1) for p in partial]
                down = [pltpu.roll(p, d, 1) for p in partial]
                for h in range(halves):
                    u = up[h] if h == halves - 1 else jnp.where(lane < LANES - d, up[h], up[h + 1])
                    w = down[h] if h == 0 else jnp.where(lane >= d, down[h], down[h - 1])
                    new[h] = new[h] - (wy[h][3 + d] * u + wy[h][3 - d] * w)
            put(i, new)

    def at0(c):
        return lambda h, i: (h * spec + c * chunk + i) * slab

    def send_edge(c):
        for up, cond in ((1, has_up), (0, has_down)):
            first = SUB // 2 + (deep - PAD if up else 0)
            land = SUB // 2 + (-PAD if up else deep)
            pl.when(cond)(functools.partial(
                push, state2.at[:, group(c), pl.ds(first, PAD)],
                state2.at[:, group(c), pl.ds(land, PAD)],
                me + (shift if up else -shift), b_send.at[up], b_recv.at[up, c]))

    def early(c):
        take(state0.at[:, group(c), pl.ds(0, rows)], in_recv.at[seat, c])
        pl.when(has_down)(lambda: take(state0.at[:, group(c), pl.ds(0, WIDE)], a_recv.at[1, c]))
        pl.when(has_up)(lambda: take(state0.at[:, group(c), pl.ds(0, WIDE)], a_recv.at[0, c]))
        base = at0(c)
        for q in (0, 1):
            off = passes[q][1]

            def put(i, new, off=off):
                for h in range(halves):
                    flat1[pl.ds((h * chunk + i) * slab1 + off + PAD, SUB), :] = new[h]

            step(q, chunk, flat0, lambda h, i: base(h, i) + SUB + off - PAD, None, None, put)

        def put(i, new):
            for h in range(halves):
                flat2[pl.ds((h * spec + c * chunk + i) * slab2 + SUB // 2, SUB), :] = new[h]

        step(2, chunk, flat1, lambda h, i: (h * chunk + i) * slab1, flat0,
             lambda h, i: base(h, i) + SUB, put)
        send_edge(c)

    def late(c):
        pl.when(has_down)(lambda: take(state2.at[:, group(c), pl.ds(0, PAD)], b_recv.at[1, c]))
        pl.when(has_up)(lambda: take(state2.at[:, group(c), pl.ds(0, PAD)], b_recv.at[0, c]))
        base = at0(c)

        def put(i, new):
            net, pos = None, None
            for h in range(halves):
                flat_r[pl.ds((h * spec + c * chunk + i) * deep, SUB), :] = new[h]
                p = jnp.maximum(new[h], 0.0)
                net, pos = (new[h], p) if net is None else (net + new[h], pos + p)
            part[0, pl.ds(i * SUB, SUB), :] = net
            part[1, pl.ds(i * SUB, SUB), :] = pos

        step(3, chunk, flat2, lambda h, i: (h * spec + c * chunk + i) * slab2 + SUB // 2 - PAD,
             flat0, lambda h, i: base(h, i) + SUB, put)
        for k in range(1, span * halves):
            m = (my_lev + k) % (span * halves)
            push(result.at[m % halves, group(c), pl.ds((m // halves) * rows, rows)],
                 back.at[group(c), my_lev], mate(m // halves, m % halves),
                 out_send.at[k], out_recv.at[c])
        local(result.at[my_gy, group(c), pl.ds(seat * rows, rows)],
              back.at[group(c), my_lev], out_recv.at[c])
        acc = stat[...]
        for o in range(2):
            tot = part[o, pl.ds(0, SUB, stride=SUB), :]
            for r in range(1, SUB):
                tot = tot + part[o, pl.ds(r, SUB, stride=SUB), :]
            acc = jnp.where(lane == c + o * (LANES // 2), jnp.sum(tot, axis=1, keepdims=True), acc)
        stat[...] = acc

    def solve(c):
        take(back.at[group(c)], out_recv.at[c])
        for i in range(chunk):
            base = (c * chunk + i) * lev * rows
            tiles = [jnp.maximum(flat_b[pl.ds(base + o * SUB, SUB), :], 0.0) for o in range(pairs)]
            swaps = [flip(t) for t in tiles]
            for o in range(pairs):
                acc = None
                for k in range(pairs):
                    term = mats[o][k][0] * tiles[k] + mats[o][k][1] * swaps[k]
                    acc = term if acc is None else acc + term
                flat_b[pl.ds(base + o * SUB, SUB), :] = acc

    @pl.loop(0, chunks + LAG_U)
    def _(i):
        @pl.when(i < chunks)
        def _():
            for k in range(1, span):
                at = (seat + k) % span
                take(state0.at[:, group(i), pl.ds(0, rows)], in_recv.at[at, i])
            send_relay(i)
            pl.when(i + AHEAD < chunks)(lambda: send_direct(i + AHEAD))

        @pl.when((i >= LAG_A) & (i < LAG_A + chunks))
        def _():
            early(i - LAG_A)

        @pl.when((i >= LAG_B) & (i < LAG_B + chunks))
        def _():
            late(i - LAG_B)

        @pl.when(i == LAG_B + chunks - 1)
        def _():
            def send_stat(k, carry):
                dev = (k + me) % n
                push(stat, stats.at[me], dev, s_send, s_recv)
                return carry

            lax.fori_loop(1, n, send_stat, 0)
            stats[pl.ds(me, 1)] = stat[...][None]

        @pl.when(i >= LAG_U)
        def _():
            solve(i - LAG_U)

    for_winds(lambda o, lv, dev, at: take(wrecv.at[0], w_send.at[o, lv]))
    whole = state0.at[0, :, pl.ds(0, rows)]
    for k in range(1, span * halves):
        take(whole, in_send.at[k])
        take(whole, out_send.at[k])

    def drain(up, at):
        _, count, _ = reach(at, up)
        if count > 0:
            for h in range(halves):
                take(state0.at[0, :, pl.ds(0, count)], d_send.at[up, h])
        total = sum(reach(other, up)[1] for other in range(span) if other != at)
        if total > 0:
            take(state0.at[:, :, pl.ds(0, total)], r_send.at[up])

    each_way(drain)
    for up, cond in ((1, has_up), (0, has_down)):
        pl.when(cond)(functools.partial(take, state2.at[:, :, pl.ds(0, PAD)], b_send.at[up]))

    others = stats.at[pl.ds(0, n - 1)]
    take(others, s_send)
    take(others, s_recv)
    total = stats[0]
    for k in range(1, n):
        total = total + stats[k]
    quotient = total / pltpu.roll(total, LANES // 2, 1)
    for c in range(chunks):
        scal[pl.ds(c * SUB, SUB), :] = jnp.broadcast_to(quotient[:, c:c + 1], (SUB, LANES))

    def mixed(s, scale, o):
        at = pl.ds(s * lev * rows + o * SUB, SUB)
        return scale * flat_b[at, :] + out_ref[at, :]

    m0 = [mixed(0, scal[0:1, :], o) for o in range(pairs)]
    above = zero
    fades = [None] * pairs
    for o in range(pairs - 1, -1, -1):
        turn = flip(m0[o])
        col = above + 0.5 * m0[o] + jnp.where(low, turn, 0.0)
        fades[o] = jnp.exp((-0.5 / lev) * col)
        above = above + (m0[o] + turn)

    @pl.loop(0, chunks)
    def _(c):
        for i in range(chunk):
            s = c * chunk + i
            scale = scal[pl.ds(c * SUB + i, 1), :]
            rate = rate_ref[s]
            for o in range(pairs):
                out_ref[pl.ds(s * lev * rows + o * SUB, SUB), :] = (
                    mixed(s, scale, o) * jnp.exp(-(rate * fades[o])))


def per_device(gx_n, halves, conc, winds, diffusivity, emission, photo_rate):
    spec, lev, rows, lanes = conc.shape
    span = lev // halves
    assert span * halves == lev and gx_n % span == 0 and lev % 2 == 0
    assert lanes == LANES and 2 * rows == SUB and span * rows == SUB and spec % 2 == 0
    n = gx_n * halves
    chunk = max(d for d in range(1, SUB + 1) if spec % d == 0)
    chunks = spec // chunk
    assert chunks <= LANES // 2
    deep = span * rows
    dims = (spec, lev, rows, halves, gx_n, span, chunk)
    f32 = jnp.float32
    hbm = pl.BlockSpec(memory_space=pl.ANY)
    dma = pltpu.SemaphoreType.DMA
    slots = (span + 2) * halves
    out = pl.pallas_call(
        functools.partial(kernel, dims),
        out_shape=pltpu.VMEM((spec * lev * rows, lanes), f32),
        in_specs=[hbm] * 4 + [pl.BlockSpec(memory_space=pltpu.SMEM)],
        out_specs=pl.BlockSpec(memory_space=pltpu.VMEM),
        scratch_shapes=[
            pltpu.VMEM((lev - 1, rows, lanes), f32),
            pltpu.VMEM((spec * rows, lanes), f32),
            pltpu.VMEM((halves, spec, deep + 2 * SUB, lanes), f32),
            pltpu.VMEM((halves, chunk, 2 * SUB, lanes), f32),
            pltpu.VMEM((halves, spec, 2 * SUB, lanes), f32),
            pltpu.VMEM((halves, spec, deep, lanes), f32),
            pltpu.VMEM((spec, lev, rows, lanes), f32),
            pltpu.VMEM((slots, 2, rows, lanes), f32),
            pltpu.VMEM((2, halves, deep + 2 * SUB, lanes), f32),
            pltpu.VMEM((4, halves, 14, SUB, lanes), f32),
            pltpu.VMEM((2, SUB * SUB, lanes), f32),
            pltpu.VMEM((SUB, lanes), f32),
            pltpu.VMEM((n, SUB, lanes), f32),
            pltpu.VMEM((chunks * SUB, lanes), f32),
            dma((2,)),
            dma((3, lev)), dma((slots,)),
            dma((lev,)), dma((span, chunks)),
            dma((2, halves)), dma((2,)), dma((2, chunks)),
            dma((2,)), dma((2, chunks)),
            dma((lev,)), dma((chunks,)),
            dma(()), dma(()),
        ],
        compiler_params=pltpu.CompilerParams(collective_id=0, has_side_effects=True),
    )(
        conc,
        winds,
        diffusivity,
        emission.reshape(spec * rows, lanes),
        photo_rate,
    )
    return out.reshape(spec, lev, rows, lanes)


def solution(mesh):
    halves = mesh.shape["gy"]
    gx_n = mesh.shape["gx"]
    return jax.shard_map(
        functools.partial(per_device, gx_n, halves),
        mesh=mesh,
        in_specs=(
            P(None, None, ("member", "gx"), "gy"),
            P(None, None, ("member", "gx"), "gy"),
            P(None, ("member", "gx"), "gy"),
            P(None, ("member", "gx"), "gy"),
            P(),
        ),
        out_specs=P(None, None, ("member", "gx"), "gy"),
        check_vma=False,
    )
```

```python
import functools

import jax
import jax.numpy as jnp
from jax import lax
from jax.experimental import pallas as pl
from jax.experimental.pallas import tpu as pltpu
from jax.sharding import PartitionSpec as P

BETAS = (1.0 / 3.0, 0.5, 1.0)
SUB = 8
LANES = 128
PAD = 3
WIDE = 2 * PAD
AHEAD = 6
LAG_A = 5
LAG_B = 10
LAG_U = 15
WIDTH = 11
MESH = pl.DeviceIdType.MESH


def stencil_weights(km, kp):
    def face(k):
        k = k / 60.0
        a = jnp.abs(k)
        return (
            k + a,
            -8.0 * k - 5.0 * a,
            37.0 * k + 10.0 * a,
            37.0 * k - 10.0 * a,
            -8.0 * k + 5.0 * a,
            k - a,
        )

    m, p = face(km), face(kp)
    return [-m[0]] + [p[j] - m[j + 1] for j in range(5)] + [p[5]]


def kernel(dims, conc_hbm, wind_hbm, diff_hbm, emis_hbm, rate_hbm, out_ref,
           rate_ref, diff_ref, emis_ref, state0, state1, state2, result, back,
           wrecv, cbuf, wts, part, stat, stats, scal,
           load_sem, w_send, w_recv, in_send, in_recv, d_send, r_send, a_recv,
           b_send, b_recv, out_send, out_recv, s_send, s_recv):
    spec, lev, rows, halves, gx_n, span, chunk = dims
    n = gx_n * halves
    chunks = spec // chunk
    groups = -(-chunk // SUB)
    deep = span * rows
    crews = gx_n // span
    slab, slab1, slab2 = deep + 2 * SUB, 2 * SUB, 2 * SUB
    my_gx, my_gy = lax.axis_index("gx"), lax.axis_index("gy")
    me = my_gx * halves + my_gy
    crew, seat = my_gx // span, my_gx % span
    my_lev = seat * halves + my_gy
    has_down, has_up = crew > 0, crew < crews - 1
    shift = span * halves

    def where_is(dev):
        return {"gx": dev // halves, "gy": dev % halves}

    def mate(at, half):
        return (crew * span + at) * halves + half

    barrier = pltpu.get_barrier_semaphore()

    def greet(k, carry):
        pl.semaphore_signal(barrier, inc=1, device_id=where_is((me + n - k) % n), device_id_type=MESH)
        return carry

    lax.fori_loop(1, n, greet, 0)
    loads = [pltpu.make_async_copy(src, dst, load_sem.at[i]) for i, (src, dst) in enumerate(
        ((diff_hbm, diff_ref), (emis_hbm, emis_ref), (rate_hbm, rate_ref)))]
    for load in loads:
        load.start()

    def push(src, dst, dev, s_sem, r_sem):
        pltpu.make_async_remote_copy(
            src_ref=src, dst_ref=dst, send_sem=s_sem, recv_sem=r_sem,
            device_id=where_is(dev), device_id_type=MESH).start()

    def local(src, dst, r_sem):
        pltpu.make_async_copy(src, dst, r_sem).start()

    def take(like, sem):
        pltpu.make_async_copy(like, like, sem).wait()

    def group(c):
        return pl.ds(c * chunk, chunk)

    flat0 = state0.reshape(halves * spec * slab, LANES)
    flat1 = state1.reshape(halves * chunk * slab1, LANES)
    flat2 = state2.reshape(halves * spec * slab2, LANES)
    flat_r = result.reshape(halves * spec * deep, LANES)
    flat_b = back.reshape(spec * lev * rows, LANES)
    zero = jnp.zeros((SUB, LANES), jnp.float32)
    few = jnp.zeros((SUB // 2, LANES), jnp.float32)

    pl.semaphore_wait(barrier, n - 1)

    own_rows = pl.ds(SUB + seat * rows, rows)

    def send_in(c):
        dst = state0.at[my_gy, group(c), own_rows]
        for k in range(1, span):
            at = (seat + k) % span
            for h in range(halves):
                push(conc_hbm.at[group(c), at * halves + h], dst, mate(at, h),
                     in_send.at[k * halves + h], in_recv.at[seat, c])
        for k in range(1, halves):
            h = (my_gy + k) % halves
            push(conc_hbm.at[group(c), seat * halves + h], dst, mate(seat, h),
                 in_send.at[k], in_recv.at[seat, c])
        local(conc_hbm.at[group(c), my_lev], dst, in_recv.at[seat, c])

    def reach(at, up):
        if up:
            first = max(0, deep - WIDE - at * rows)
            return first, rows - first, SUB - deep + at * rows + first
        return 0, max(0, min(rows, WIDE - at * rows)), SUB + deep + at * rows

    def each_way(act):
        for up, cond in ((1, has_up), (0, has_down)):
            for at in range(span):
                pl.when(cond & (seat == at))(functools.partial(act, up, at))

    def send_direct(c):
        def act(up, at):
            first, count, land = reach(at, up)
            if count > 0:
                for h in range(halves):
                    push(conc_hbm.at[group(c), at * halves + h, pl.ds(first, count)],
                         state0.at[my_gy, group(c), pl.ds(land, count)],
                         mate(at, h) + (shift if up else -shift),
                         d_send.at[up, h], a_recv.at[up, c])

        each_way(act)

    def send_relay(c):
        def act(up, at):
            for other in range(span):
                first, count, land = reach(other, up)
                if other != at and count > 0:
                    push(state0.at[:, group(c), pl.ds(SUB + other * rows + first, count)],
                         state0.at[:, group(c), pl.ds(land, count)],
                         me + (shift if up else -shift), r_send.at[up], a_recv.at[up, c])

        each_way(act)

    sides = ((0, None, None), (1, has_up & (seat == span - 1), 0),
             (-1, has_down & (seat == 0), span + 1))

    def for_winds(act):
        for o, (step, cond, slot) in enumerate(sides):
            at = seat + 1 if slot is None else slot
            for lv in range(lev):
                dev = mate(lv // halves, lv % halves) + step * shift
                if cond is None:
                    pl.when(dev != me)(functools.partial(act, o, lv, dev, at))
                else:
                    pl.when(cond)(functools.partial(act, o, lv, dev, at))

    for_winds(lambda o, lv, dev, at: push(
        wind_hbm.at[:, lv], wrecv.at[at * halves + my_gy], dev, w_send.at[o, lv],
        w_recv.at[at * halves + my_gy]))
    local(wind_hbm.at[:, my_lev], wrecv.at[(seat + 1) * halves + my_gy],
          w_recv.at[(seat + 1) * halves + my_gy])

    @pl.loop(0, chunks)
    def _(c):
        pl.when(c < AHEAD)(lambda: send_direct(c))
        send_in(c)

    def clear(first0, first2):
        @pl.loop(0, halves * chunks)
        def _(i):
            for k in range(chunk):
                flat0[pl.ds((i * chunk + k) * slab + first0, SUB), :] = zero
                flat2[pl.ds((i * chunk + k) * slab2 + first2, SUB // 2), :] = few

    pl.when(crew == 0)(lambda: clear(0, 0))
    pl.when(crew == crews - 1)(lambda: clear(SUB + deep, SUB // 2 + deep))
    for h in range(halves):
        for c in range(2):
            cbuf[c, h, 0:SUB, :] = zero
            cbuf[c, h, SUB + deep:2 * SUB + deep, :] = zero
    part[...] = jnp.zeros_like(part)
    stat[...] = zero

    lane = lax.broadcasted_iota(jnp.int32, (SUB, LANES), 1)
    sub = lax.broadcasted_iota(jnp.int32, (SUB, LANES), 0)

    for load in loads:
        load.wait()
    ks = [diff_ref[lv] for lv in range(lev - 1)]
    none = jnp.zeros((rows, LANES), jnp.float32)
    lower, upper = [none] + ks, ks + [none]
    inv, ratio = [], []
    for lv in range(lev):
        pivot = 1.0 + lower[lv] + upper[lv]
        if lv:
            pivot = pivot - lower[lv] * ratio[-1]
        inv.append(1.0 / pivot)
        ratio.append(upper[lv] * inv[lv])
    inverse = [[None] * lev for _ in range(lev)]
    for j in range(lev):
        val = [none] * lev
        for lv in range(j, lev):
            val[lv] = inv[lv] if lv == j else lower[lv] * val[lv - 1] * inv[lv]
        for lv in range(lev - 1, -1, -1):
            inverse[lv][j] = val[lv] if lv == lev - 1 else val[lv] + ratio[lv] * inverse[lv + 1][j]
    pairs = lev // 2

    def duo(a, b):
        return jnp.concatenate([a, b], axis=0)

    mats = [[(duo(inverse[2 * o][2 * i], inverse[2 * o + 1][2 * i + 1]),
              duo(inverse[2 * o][2 * i + 1], inverse[2 * o + 1][2 * i]))
             for i in range(pairs)] for o in range(pairs)]
    first_col = [duo(inverse[2 * o][0], inverse[2 * o + 1][0]) for o in range(pairs)]

    def flip(v):
        return pltpu.roll(v, SUB // 2, 0)

    low = sub < SUB // 2

    @pl.loop(0, spec // 2)
    def _(s):
        e = emis_ref[pl.ds(s * SUB, SUB), :]
        f = flip(e)
        for k, v in enumerate((jnp.where(low, e, f), jnp.where(low, f, e))):
            for o in range(pairs):
                out_ref[pl.ds((2 * s + k) * lev * rows + o * SUB, SUB), :] = first_col[o] * v

    def wind_in(slot):
        for h in range(halves):
            take(wrecv.at[slot * halves + h], w_recv.at[slot * halves + h])
            for c in range(2):
                base = SUB + (slot - 1) * rows
                cbuf[c, h, base:base + rows, :] = wrecv[slot * halves + h, c]

    for slot in range(1, span + 1):
        wind_in(slot)
    pl.when(has_down)(lambda: wind_in(0))
    pl.when(has_up)(lambda: wind_in(span + 1))

    passes = ((0, -PAD), (0, deep - SUB + PAD), (1, 0), (2, 0))
    for q, (s, r0) in enumerate(passes):
        at_row = crew * deep + r0 + sub
        inside = (at_row >= 0) & (at_row < crews * deep)
        for h in range(halves):
            here, left, right = (cbuf[0, h, SUB + r0 + d:2 * SUB + r0 + d, :] for d in (0, -1, 1))
            for j, w in enumerate(stencil_weights(0.5 * (left + here), 0.5 * (here + right))):
                wts[q, h, j] = jnp.where(inside, w, 0.0) * BETAS[s]
        cy = [cbuf[1, h, SUB + r0:2 * SUB + r0, :] for h in range(halves)]
        for h in range(halves):
            nxt = pltpu.roll(cy[h + 1], LANES - 1, 1) if h + 1 < halves else zero
            prv = pltpu.roll(cy[h - 1], 1, 1) if h > 0 else zero
            up = jnp.where(lane < LANES - 1, pltpu.roll(cy[h], LANES - 1, 1), nxt)
            down = jnp.where(lane >= 1, pltpu.roll(cy[h], 1, 1), prv)
            ws = stencil_weights(0.5 * (down + cy[h]), 0.5 * (cy[h] + up))
            for j, w in enumerate(ws):
                d = j - 3
                if d > 0 and h == halves - 1:
                    w = jnp.where(lane < LANES - d, w, 0.0)
                if d < 0 and h == 0:
                    w = jnp.where(lane >= -d, w, 0.0)
                wts[q, h, 7 + j] = w * BETAS[s]

    def step(q, count, src, src_at, start, start_at, put):
        wx = [[wts[q, h, j] for j in range(7)] for h in range(halves)]
        wy = [[wts[q, h, 7 + j] for j in range(7)] for h in range(halves)]
        for i in range(count):
            partial, new = [], []
            for h in range(halves):
                base = src_at(h, i)
                mid = None
                acc = None
                for j in range(7):
                    v = src[pl.ds(base + j, SUB), :]
                    if j == PAD:
                        mid = v
                    acc = wx[h][j] * v if acc is None else acc + wx[h][j] * v
                p = mid - acc
                partial.append(p)
                begin = mid if start is None else start[pl.ds(start_at(h, i), SUB), :]
                new.append(begin - acc - wy[h][3] * p)
            for d in (1, 2, 3):
                up = [pltpu.roll(p, LANES - d, 1) for p in partial]
                down = [pltpu.roll(p, d, 1) for p in partial]
                for h in range(halves):
                    u = up[h] if h == halves - 1 else jnp.where(lane < LANES - d, up[h], up[h + 1])
                    w = down[h] if h == 0 else jnp.where(lane >= d, down[h], down[h - 1])
                    new[h] = new[h] - (wy[h][3 + d] * u + wy[h][3 - d] * w)
            put(i, new)

    def at0(c):
        return lambda h, i: (h * spec + c * chunk + i) * slab

    def send_edge(c):
        for up, cond in ((1, has_up), (0, has_down)):
            first = SUB // 2 + (deep - PAD if up else 0)
            land = SUB // 2 + (-PAD if up else deep)
            pl.when(cond)(functools.partial(
                push, state2.at[:, group(c), pl.ds(first, PAD)],
                state2.at[:, group(c), pl.ds(land, PAD)],
                me + (shift if up else -shift), b_send.at[up], b_recv.at[up, c]))

    def early(c):
        take(state0.at[:, group(c), pl.ds(0, rows)], in_recv.at[seat, c])
        pl.when(has_down)(lambda: take(state0.at[:, group(c), pl.ds(0, WIDE)], a_recv.at[1, c]))
        pl.when(has_up)(lambda: take(state0.at[:, group(c), pl.ds(0, WIDE)], a_recv.at[0, c]))
        base = at0(c)
        for q in (0, 1):
            off = passes[q][1]

            def put(i, new, off=off):
                for h in range(halves):
                    flat1[pl.ds((h * chunk + i) * slab1 + off + PAD, SUB), :] = new[h]

            step(q, chunk, flat0, lambda h, i: base(h, i) + SUB + off - PAD, None, None, put)

        def put(i, new):
            for h in range(halves):
                flat2[pl.ds((h * spec + c * chunk + i) * slab2 + SUB // 2, SUB), :] = new[h]

        step(2, chunk, flat1, lambda h, i: (h * chunk + i) * slab1, flat0,
             lambda h, i: base(h, i) + SUB, put)
        send_edge(c)

    def late(c):
        pl.when(has_down)(lambda: take(state2.at[:, group(c), pl.ds(0, PAD)], b_recv.at[1, c]))
        pl.when(has_up)(lambda: take(state2.at[:, group(c), pl.ds(0, PAD)], b_recv.at[0, c]))
        base = at0(c)

        def put(i, new):
            net, pos = None, None
            for h in range(halves):
                flat_r[pl.ds((h * spec + c * chunk + i) * deep, SUB), :] = new[h]
                p = jnp.maximum(new[h], 0.0)
                net, pos = (new[h], p) if net is None else (net + new[h], pos + p)
            part[0, pl.ds(i * SUB, SUB), :] = net
            part[1, pl.ds(i * SUB, SUB), :] = pos

        step(3, chunk, flat2, lambda h, i: (h * spec + c * chunk + i) * slab2 + SUB // 2 - PAD,
             flat0, lambda h, i: base(h, i) + SUB, put)
        acc = stat[...]
        for o in range(2):
            for g in range(groups):
                first = g * SUB * SUB
                tot = part[o, pl.ds(first, SUB, stride=SUB), :]
                for r in range(1, SUB):
                    tot = tot + part[o, pl.ds(first + r, SUB, stride=SUB), :]
                acc = jnp.where(lane == c * groups + g + o * (LANES // 2),
                                jnp.sum(tot, axis=1, keepdims=True), acc)
        stat[...] = acc

        @pl.when(c == chunks - 1)
        def _():
            def send_stat(k, carry):
                dev = (k + me) % n
                push(stat, stats.at[me], dev, s_send, s_recv)
                return carry

            lax.fori_loop(1, n, send_stat, 0)
            stats[pl.ds(me, 1)] = stat[...][None]

        for k in range(1, span * halves):
            m = (my_lev + k) % (span * halves)
            push(result.at[m % halves, group(c), pl.ds((m // halves) * rows, rows)],
                 back.at[group(c), my_lev], mate(m // halves, m % halves),
                 out_send.at[k], out_recv.at[c])
        local(result.at[my_gy, group(c), pl.ds(seat * rows, rows)],
              back.at[group(c), my_lev], out_recv.at[c])

    def solve(c):
        take(back.at[group(c)], out_recv.at[c])
        for i in range(chunk):
            base = (c * chunk + i) * lev * rows
            tiles = [jnp.maximum(flat_b[pl.ds(base + o * SUB, SUB), :], 0.0) for o in range(pairs)]
            swaps = [flip(t) for t in tiles]
            for o in range(pairs):
                acc = None
                for k in range(pairs):
                    term = mats[o][k][0] * tiles[k] + mats[o][k][1] * swaps[k]
                    acc = term if acc is None else acc + term
                flat_b[pl.ds(base + o * SUB, SUB), :] = acc

    @pl.loop(0, chunks + LAG_U)
    def _(i):
        @pl.when(i < chunks)
        def _():
            for k in range(1, span):
                at = (seat + k) % span
                take(state0.at[:, group(i), pl.ds(0, rows)], in_recv.at[at, i])
            send_relay(i)
            pl.when(i + AHEAD < chunks)(lambda: send_direct(i + AHEAD))

        @pl.when((i >= LAG_A) & (i < LAG_A + chunks))
        def _():
            early(i - LAG_A)

        @pl.when((i >= LAG_B) & (i < LAG_B + chunks))
        def _():
            late(i - LAG_B)

        @pl.when(i >= LAG_U)
        def _():
            solve(i - LAG_U)

    for_winds(lambda o, lv, dev, at: take(wrecv.at[0], w_send.at[o, lv]))
    whole = state0.at[0, :, pl.ds(0, rows)]
    for k in range(1, span * halves):
        take(whole, in_send.at[k])
        take(whole, out_send.at[k])

    def drain(up, at):
        _, count, _ = reach(at, up)
        if count > 0:
            for h in range(halves):
                take(state0.at[0, :, pl.ds(0, count)], d_send.at[up, h])
        total = sum(reach(other, up)[1] for other in range(span) if other != at)
        if total > 0:
            take(state0.at[:, :, pl.ds(0, total)], r_send.at[up])

    each_way(drain)
    for up, cond in ((1, has_up), (0, has_down)):
        pl.when(cond)(functools.partial(take, state2.at[:, :, pl.ds(0, PAD)], b_send.at[up]))

    others = stats.at[pl.ds(0, n - 1)]
    take(others, s_send)
    take(others, s_recv)
    total = stats[0]
    for k in range(1, n):
        total = total + stats[k]
    quotient = total / pltpu.roll(total, LANES // 2, 1)
    for c in range(chunks * groups):
        scal[pl.ds(c * SUB, SUB), :] = jnp.broadcast_to(quotient[:, c:c + 1], (SUB, LANES))

    def mixed(s, scale, o):
        at = pl.ds(s * lev * rows + o * SUB, SUB)
        return scale * flat_b[at, :] + out_ref[at, :]

    m0 = [mixed(0, scal[0:1, :], o) for o in range(pairs)]
    above = zero
    fades = [None] * pairs
    for o in range(pairs - 1, -1, -1):
        turn = flip(m0[o])
        col = above + 0.5 * m0[o] + jnp.where(low, turn, 0.0)
        fades[o] = jnp.exp((-0.5 / lev) * col)
        above = above + (m0[o] + turn)

    @pl.loop(0, chunks)
    def _(c):
        for i in range(chunk):
            s = c * chunk + i
            scale = scal[pl.ds(c * groups * SUB + i, 1), :]
            rate = rate_ref[s]
            for o in range(pairs):
                out_ref[pl.ds(s * lev * rows + o * SUB, SUB), :] = (
                    mixed(s, scale, o) * jnp.exp(-(rate * fades[o])))


def per_device(gx_n, halves, conc, winds, diffusivity, emission, photo_rate):
    spec, lev, rows, lanes = conc.shape
    span = lev // halves
    assert span * halves == lev and gx_n % span == 0 and lev % 2 == 0
    assert lanes == LANES and 2 * rows == SUB and span * rows == SUB and spec % 2 == 0
    n = gx_n * halves
    chunk = max(d for d in range(1, WIDTH + 1) if spec % d == 0)
    chunks = spec // chunk
    groups = -(-chunk // SUB)
    assert chunks * groups <= LANES // 2
    deep = span * rows
    dims = (spec, lev, rows, halves, gx_n, span, chunk)
    f32 = jnp.float32
    hbm = pl.BlockSpec(memory_space=pl.ANY)
    dma = pltpu.SemaphoreType.DMA
    slots = (span + 2) * halves
    out = pl.pallas_call(
        functools.partial(kernel, dims),
        out_shape=pltpu.VMEM((spec * lev * rows, lanes), f32),
        in_specs=[hbm] * 5,
        out_specs=pl.BlockSpec(memory_space=pltpu.VMEM),
        scratch_shapes=[
            pltpu.SMEM((spec,), f32),
            pltpu.VMEM((lev - 1, rows, lanes), f32),
            pltpu.VMEM((spec * rows, lanes), f32),
            pltpu.VMEM((halves, spec, deep + 2 * SUB, lanes), f32),
            pltpu.VMEM((halves, chunk, 2 * SUB, lanes), f32),
            pltpu.VMEM((halves, spec, 2 * SUB, lanes), f32),
            pltpu.VMEM((halves, spec, deep, lanes), f32),
            pltpu.VMEM((spec, lev, rows, lanes), f32),
            pltpu.VMEM((slots, 2, rows, lanes), f32),
            pltpu.VMEM((2, halves, deep + 2 * SUB, lanes), f32),
            pltpu.VMEM((4, halves, 14, SUB, lanes), f32),
            pltpu.VMEM((2, groups * SUB * SUB, lanes), f32),
            pltpu.VMEM((SUB, lanes), f32),
            pltpu.VMEM((n, SUB, lanes), f32),
            pltpu.VMEM((chunks * groups * SUB, lanes), f32),
            dma((3,)),
            dma((3, lev)), dma((slots,)),
            dma((lev,)), dma((span, chunks)),
            dma((2, halves)), dma((2,)), dma((2, chunks)),
            dma((2,)), dma((2, chunks)),
            dma((lev,)), dma((chunks,)),
            dma(()), dma(()),
        ],
        compiler_params=pltpu.CompilerParams(collective_id=0, has_side_effects=True),
    )(
        conc,
        winds,
        diffusivity,
        emission.reshape(spec * rows, lanes),
        photo_rate,
    )
    return out.reshape(spec, lev, rows, lanes)


def solution(mesh):
    halves = mesh.shape["gy"]
    gx_n = mesh.shape["gx"]
    return jax.shard_map(
        functools.partial(per_device, gx_n, halves),
        mesh=mesh,
        in_specs=(
            P(None, None, ("member", "gx"), "gy"),
            P(None, None, ("member", "gx"), "gy"),
            P(None, ("member", "gx"), "gy"),
            P(None, ("member", "gx"), "gy"),
            P(),
        ),
        out_specs=P(None, None, ("member", "gx"), "gy"),
        check_vma=False,
    )
```

```python
import functools

import jax
import jax.numpy as jnp
from jax import lax
from jax.experimental import pallas as pl
from jax.experimental.pallas import tpu as pltpu
from jax.sharding import PartitionSpec as P

BETAS = (1.0 / 3.0, 0.5, 1.0)
SUB = 8
LANES = 128
PAD = 3
WIDE = 2 * PAD
LAG_A = 5
LAG_B = 10
LAG_U = 15
WIDTH = 11
MESH = pl.DeviceIdType.MESH


def stencil_weights(km, kp):
    def face(k):
        k = k / 60.0
        a = jnp.abs(k)
        return (
            k + a,
            -8.0 * k - 5.0 * a,
            37.0 * k + 10.0 * a,
            37.0 * k - 10.0 * a,
            -8.0 * k + 5.0 * a,
            k - a,
        )

    m, p = face(km), face(kp)
    return [-m[0]] + [p[j] - m[j + 1] for j in range(5)] + [p[5]]


def kernel(dims, conc_hbm, wind_hbm, diff_hbm, emis_hbm, rate_hbm, out_ref,
           rate_ref, diff_ref, emis_ref, state0, state1, state2, result, back,
           wrecv, cbuf, wts, part, stat, stats, scal,
           load_sem, w_send, w_recv, in_send, in_recv, own_recv, d_send, d_recv, r_send, a_recv,
           b_send, b_recv, out_send, out_recv, s_send, s_recv, token):
    spec, lev, rows, halves, gx_n, span, chunk = dims
    n = gx_n * halves
    chunks = spec // chunk
    groups = -(-chunk // SUB)
    deep = span * rows
    crews = gx_n // span
    slab, slab1, slab2 = deep + 2 * SUB, 2 * SUB, 2 * SUB
    my_gx, my_gy = lax.axis_index("gx"), lax.axis_index("gy")
    me = my_gx * halves + my_gy
    crew, seat = my_gx // span, my_gx % span
    my_lev = seat * halves + my_gy
    has_down, has_up = crew > 0, crew < crews - 1
    shift = span * halves

    def where_is(dev):
        return {"gx": dev // halves, "gy": dev % halves}

    def mate(at, half):
        return (crew * span + at) * halves + half

    barrier = pltpu.get_barrier_semaphore()

    def greet(dev):
        pl.semaphore_signal(barrier, inc=1, device_id=where_is(dev), device_id_type=MESH)

    for k in range(1, lev):
        m = (my_lev + k) % lev
        greet(mate(m // halves, m % halves))
    for cond, move in ((has_down, -shift), (has_up, shift)):
        @pl.when(cond)
        def _():
            for m in range(lev):
                greet(mate(m // halves, m % halves) + move)

    loads = [pltpu.make_async_copy(src, dst, load_sem.at[i]) for i, (src, dst) in enumerate(
        ((diff_hbm, diff_ref), (emis_hbm, emis_ref), (rate_hbm, rate_ref)))]
    for load in loads:
        load.start()

    def push(src, dst, dev, s_sem, r_sem):
        pltpu.make_async_remote_copy(
            src_ref=src, dst_ref=dst, send_sem=s_sem, recv_sem=r_sem,
            device_id=where_is(dev), device_id_type=MESH).start()

    def local(src, dst, r_sem):
        pltpu.make_async_copy(src, dst, r_sem).start()

    def take(like, sem):
        pltpu.make_async_copy(like, like, sem).wait()

    def group(c):
        return pl.ds(c * chunk, chunk)

    flat0 = state0.reshape(halves * spec * slab, LANES)
    flat1 = state1.reshape(halves * chunk * slab1, LANES)
    flat2 = state2.reshape(halves * spec * slab2, LANES)
    flat_r = result.reshape(halves * spec * deep, LANES)
    flat_b = back.reshape(spec * lev * rows, LANES)
    zero = jnp.zeros((SUB, LANES), jnp.float32)
    few = jnp.zeros((SUB // 2, LANES), jnp.float32)

    pl.semaphore_wait(barrier, lev - 1 + jnp.where(has_down, lev, 0) + jnp.where(has_up, lev, 0))

    own_rows = pl.ds(SUB + seat * rows, rows)

    def send_in(c):
        dst = state0.at[my_gy, group(c), own_rows]
        for k in range(1, span):
            at = (seat + k) % span
            for h in range(halves):
                push(conc_hbm.at[group(c), at * halves + h], dst, mate(at, h),
                     in_send.at[k * halves + h], in_recv.at[seat, c])

    def send_own():
        dst = state0.at[my_gy, :, own_rows]
        for k in range(1, halves):
            h = (my_gy + k) % halves
            push(conc_hbm.at[:, seat * halves + h], dst, mate(seat, h), in_send.at[k], own_recv)
        local(conc_hbm.at[:, my_lev], dst, own_recv)

    def reach(at, up):
        if up:
            first = max(0, deep - WIDE - at * rows)
            return first, rows - first, SUB - deep + at * rows + first
        return 0, max(0, min(rows, WIDE - at * rows)), SUB + deep + at * rows

    def each_way(act, landing=False):
        for up, cond in ((1, has_down if landing else has_up), (0, has_up if landing else has_down)):
            for at in range(span):
                pl.when(cond & (seat == at))(functools.partial(act, up, at))

    def send_direct():
        def act(up, at):
            first, count, land = reach(at, up)
            if count > 0:
                for h in range(halves):
                    push(conc_hbm.at[:, at * halves + h, pl.ds(first, count)],
                         state0.at[my_gy, :, pl.ds(land, count)],
                         mate(at, h) + (shift if up else -shift),
                         d_send.at[up, h], d_recv.at[up])

        each_way(act)

    def send_relay(c):
        def act(up, at):
            for other in range(span):
                first, count, land = reach(other, up)
                if other != at and count > 0:
                    push(state0.at[:, group(c), pl.ds(SUB + other * rows + first, count)],
                         state0.at[:, group(c), pl.ds(land, count)],
                         me + (shift if up else -shift), r_send.at[up], a_recv.at[up, c])

        each_way(act)

    sides = ((0, None, None), (1, has_up & (seat == span - 1), 0),
             (-1, has_down & (seat == 0), span + 1))

    def for_winds(act):
        for o, (step, cond, slot) in enumerate(sides):
            at = seat + 1 if slot is None else slot
            for lv in range(lev):
                dev = mate(lv // halves, lv % halves) + step * shift
                if cond is None:
                    pl.when(dev != me)(functools.partial(act, o, lv, dev, at))
                else:
                    pl.when(cond)(functools.partial(act, o, lv, dev, at))

    send_in(0)
    for_winds(lambda o, lv, dev, at: push(
        wind_hbm.at[:, lv], wrecv.at[at * halves + my_gy], dev, w_send.at[o, lv],
        w_recv.at[at * halves + my_gy]))
    local(wind_hbm.at[:, my_lev], wrecv.at[(seat + 1) * halves + my_gy],
          w_recv.at[(seat + 1) * halves + my_gy])

    send_own()

    @pl.loop(1, chunks)
    def _(c):
        send_in(c)

    send_direct()
    def clear(first0, first2):
        @pl.loop(0, halves * chunks)
        def _(i):
            for k in range(chunk):
                flat0[pl.ds((i * chunk + k) * slab + first0, SUB), :] = zero
                flat2[pl.ds((i * chunk + k) * slab2 + first2, SUB // 2), :] = few

    pl.when(crew == 0)(lambda: clear(0, 0))
    pl.when(crew == crews - 1)(lambda: clear(SUB + deep, SUB // 2 + deep))
    for h in range(halves):
        for c in range(2):
            cbuf[c, h, 0:SUB, :] = zero
            cbuf[c, h, SUB + deep:2 * SUB + deep, :] = zero
    part[...] = jnp.zeros_like(part)
    stat[...] = zero

    lane = lax.broadcasted_iota(jnp.int32, (SUB, LANES), 1)
    sub = lax.broadcasted_iota(jnp.int32, (SUB, LANES), 0)

    for load in loads:
        load.wait()
    ks = [diff_ref[lv] for lv in range(lev - 1)]
    none = jnp.zeros((rows, LANES), jnp.float32)
    lower, upper = [none] + ks, ks + [none]
    inv, ratio = [], []
    for lv in range(lev):
        pivot = 1.0 + lower[lv] + upper[lv]
        if lv:
            pivot = pivot - lower[lv] * ratio[-1]
        inv.append(1.0 / pivot)
        ratio.append(upper[lv] * inv[lv])
    inverse = [[None] * lev for _ in range(lev)]
    for j in range(lev):
        val = [none] * lev
        for lv in range(j, lev):
            val[lv] = inv[lv] if lv == j else lower[lv] * val[lv - 1] * inv[lv]
        for lv in range(lev - 1, -1, -1):
            inverse[lv][j] = val[lv] if lv == lev - 1 else val[lv] + ratio[lv] * inverse[lv + 1][j]
    pairs = lev // 2

    def duo(a, b):
        return jnp.concatenate([a, b], axis=0)

    mats = [[(duo(inverse[2 * o][2 * i], inverse[2 * o + 1][2 * i + 1]),
              duo(inverse[2 * o][2 * i + 1], inverse[2 * o + 1][2 * i]))
             for i in range(pairs)] for o in range(pairs)]
    first_col = [duo(inverse[2 * o][0], inverse[2 * o + 1][0]) for o in range(pairs)]

    def flip(v):
        return pltpu.roll(v, SUB // 2, 0)

    low = sub < SUB // 2

    @pl.loop(0, spec // 2)
    def _(s):
        e = emis_ref[pl.ds(s * SUB, SUB), :]
        f = flip(e)
        for k, v in enumerate((jnp.where(low, e, f), jnp.where(low, f, e))):
            for o in range(pairs):
                out_ref[pl.ds((2 * s + k) * lev * rows + o * SUB, SUB), :] = first_col[o] * v

    def wind_in(slot):
        for h in range(halves):
            take(wrecv.at[slot * halves + h], w_recv.at[slot * halves + h])
            for c in range(2):
                base = SUB + (slot - 1) * rows
                cbuf[c, h, base:base + rows, :] = wrecv[slot * halves + h, c]

    for slot in range(1, span + 1):
        wind_in(slot)
    pl.when(has_down)(lambda: wind_in(0))
    pl.when(has_up)(lambda: wind_in(span + 1))

    passes = ((0, -PAD), (0, deep - SUB + PAD), (1, 0), (2, 0))
    for q, (s, r0) in enumerate(passes):
        at_row = crew * deep + r0 + sub
        inside = (at_row >= 0) & (at_row < crews * deep)
        for h in range(halves):
            here, left, right = (cbuf[0, h, SUB + r0 + d:2 * SUB + r0 + d, :] for d in (0, -1, 1))
            for j, w in enumerate(stencil_weights(0.5 * (left + here), 0.5 * (here + right))):
                wts[q, h, j] = jnp.where(inside, w, 0.0) * BETAS[s]
        cy = [cbuf[1, h, SUB + r0:2 * SUB + r0, :] for h in range(halves)]
        for h in range(halves):
            nxt = pltpu.roll(cy[h + 1], LANES - 1, 1) if h + 1 < halves else zero
            prv = pltpu.roll(cy[h - 1], 1, 1) if h > 0 else zero
            up = jnp.where(lane < LANES - 1, pltpu.roll(cy[h], LANES - 1, 1), nxt)
            down = jnp.where(lane >= 1, pltpu.roll(cy[h], 1, 1), prv)
            ws = stencil_weights(0.5 * (down + cy[h]), 0.5 * (cy[h] + up))
            for j, w in enumerate(ws):
                d = j - 3
                if d > 0 and h == halves - 1:
                    w = jnp.where(lane < LANES - d, w, 0.0)
                if d < 0 and h == 0:
                    w = jnp.where(lane >= -d, w, 0.0)
                wts[q, h, 7 + j] = w * BETAS[s]

    def step(q, count, src, src_at, start, start_at, put):
        wx = [[wts[q, h, j] for j in range(7)] for h in range(halves)]
        wy = [[wts[q, h, 7 + j] for j in range(7)] for h in range(halves)]
        for i in range(count):
            partial, new = [], []
            for h in range(halves):
                base = src_at(h, i)
                mid = None
                acc = None
                for j in range(7):
                    v = src[pl.ds(base + j, SUB), :]
                    if j == PAD:
                        mid = v
                    acc = wx[h][j] * v if acc is None else acc + wx[h][j] * v
                p = mid - acc
                partial.append(p)
                begin = mid if start is None else start[pl.ds(start_at(h, i), SUB), :]
                new.append(begin - acc - wy[h][3] * p)
            for d in (1, 2, 3):
                up = [pltpu.roll(p, LANES - d, 1) for p in partial]
                down = [pltpu.roll(p, d, 1) for p in partial]
                for h in range(halves):
                    u = up[h] if h == halves - 1 else jnp.where(lane < LANES - d, up[h], up[h + 1])
                    w = down[h] if h == 0 else jnp.where(lane >= d, down[h], down[h - 1])
                    new[h] = new[h] - (wy[h][3 + d] * u + wy[h][3 - d] * w)
            put(i, new)

    def at0(c):
        return lambda h, i: (h * spec + c * chunk + i) * slab

    def send_edge(c):
        for up, cond in ((1, has_up), (0, has_down)):
            first = SUB // 2 + (deep - PAD if up else 0)
            land = SUB // 2 + (-PAD if up else deep)
            pl.when(cond)(functools.partial(
                push, state2.at[:, group(c), pl.ds(first, PAD)],
                state2.at[:, group(c), pl.ds(land, PAD)],
                me + (shift if up else -shift), b_send.at[up], b_recv.at[up, c]))

    def arrive(up, at):
        count = reach(at, up)[1]
        if count > 0:
            take(state0.at[:, :, pl.ds(0, count)], d_recv.at[up])

    def arrive_relay(c, up, at):
        total = sum(reach(other, up)[1] for other in range(span) if other != at)
        if total > 0:
            take(state0.at[:, group(c), pl.ds(0, total)], a_recv.at[up, c])

    def early(c):

        @pl.when(c == 0)
        def _():
            take(state0.at[:, :, pl.ds(0, rows)], own_recv)
            each_way(arrive, True)

        each_way(functools.partial(arrive_relay, c), True)
        base = at0(c)
        for q in (0, 1):
            off = passes[q][1]

            def put(i, new, off=off):
                for h in range(halves):
                    flat1[pl.ds((h * chunk + i) * slab1 + off + PAD, SUB), :] = new[h]

            step(q, chunk, flat0, lambda h, i: base(h, i) + SUB + off - PAD, None, None, put)

        def put(i, new):
            for h in range(halves):
                flat2[pl.ds((h * spec + c * chunk + i) * slab2 + SUB // 2, SUB), :] = new[h]

        step(2, chunk, flat1, lambda h, i: (h * chunk + i) * slab1, flat0,
             lambda h, i: base(h, i) + SUB, put)
        send_edge(c)

    def late(c):
        pl.when(has_down)(lambda: take(state2.at[:, group(c), pl.ds(0, PAD)], b_recv.at[1, c]))
        pl.when(has_up)(lambda: take(state2.at[:, group(c), pl.ds(0, PAD)], b_recv.at[0, c]))
        base = at0(c)

        def put(i, new):
            net, pos = None, None
            for h in range(halves):
                flat_r[pl.ds((h * spec + c * chunk + i) * deep, SUB), :] = new[h]
                p = jnp.maximum(new[h], 0.0)
                net, pos = (new[h], p) if net is None else (net + new[h], pos + p)
            part[0, pl.ds(i * SUB, SUB), :] = net
            part[1, pl.ds(i * SUB, SUB), :] = pos

        step(3, chunk, flat2, lambda h, i: (h * spec + c * chunk + i) * slab2 + SUB // 2 - PAD,
             flat0, lambda h, i: base(h, i) + SUB, put)
        acc = stat[...]
        for o in range(2):
            for g in range(groups):
                first = g * SUB * SUB
                tot = part[o, pl.ds(first, SUB, stride=SUB), :]
                for r in range(1, SUB):
                    tot = tot + part[o, pl.ds(first + r, SUB, stride=SUB), :]
                acc = jnp.where(lane == c * groups + g + o * (LANES // 2),
                                jnp.sum(tot, axis=1, keepdims=True), acc)
        stat[...] = acc

        @pl.when(c == chunks - 1)
        def _():
            def send_stat(k, carry):
                dev = (k + me) % n
                push(stat, stats.at[me], dev, s_send, s_recv)
                return carry

            lax.fori_loop(1, n, send_stat, 0)
            stats[pl.ds(me, 1)] = stat[...][None]

        for k in range(1, span * halves):
            m = (my_lev + k) % (span * halves)
            push(result.at[m % halves, group(c), pl.ds((m // halves) * rows, rows)],
                 back.at[group(c), my_lev], mate(m // halves, m % halves),
                 out_send.at[k], out_recv.at[c])
        local(result.at[my_gy, group(c), pl.ds(seat * rows, rows)],
              back.at[group(c), my_lev], out_recv.at[c])

    def solve(c):
        take(back.at[group(c)], out_recv.at[c])
        for i in range(chunk):
            base = (c * chunk + i) * lev * rows
            tiles = [jnp.maximum(flat_b[pl.ds(base + o * SUB, SUB), :], 0.0) for o in range(pairs)]
            swaps = [flip(t) for t in tiles]
            for o in range(pairs):
                acc = None
                for k in range(pairs):
                    term = mats[o][k][0] * tiles[k] + mats[o][k][1] * swaps[k]
                    acc = term if acc is None else acc + term
                flat_b[pl.ds(base + o * SUB, SUB), :] = acc

    def pass_on(up):
        pl.semaphore_signal(token.at[up], inc=1, device_id=where_is(me + (shift if up else -shift)),
                            device_id_type=MESH)

    pl.when(has_up & (crew == 0))(lambda: pass_on(1))
    pl.when(has_down & (crew == crews - 1))(lambda: pass_on(0))

    @pl.loop(0, chunks + LAG_U)
    def _(i):
        for up, cond, on, turn in ((1, has_down, has_up, crew), (0, has_up, has_down, crews - 1 - crew)):
            @pl.when(cond & (i == turn))
            def _():
                pl.semaphore_wait(token.at[up], 1)
                pl.when(on)(functools.partial(pass_on, up))

        @pl.when(i < chunks)
        def _():
            for k in range(1, span):
                at = (seat + k) % span
                take(state0.at[:, group(i), pl.ds(0, rows)], in_recv.at[at, i])
            send_relay(i)

        @pl.when((i >= LAG_A) & (i < LAG_A + chunks))
        def _():
            early(i - LAG_A)

        @pl.when((i >= LAG_B) & (i < LAG_B + chunks))
        def _():
            late(i - LAG_B)

        @pl.when(i >= LAG_U)
        def _():
            solve(i - LAG_U)

    for_winds(lambda o, lv, dev, at: take(wrecv.at[0], w_send.at[o, lv]))
    whole = state0.at[0, :, pl.ds(0, rows)]
    for k in range(1, span * halves):
        take(whole, in_send.at[k])
        take(whole, out_send.at[k])

    def drain(up, at):
        _, count, _ = reach(at, up)
        if count > 0:
            for h in range(halves):
                take(state0.at[0, :, pl.ds(0, count)], d_send.at[up, h])
        total = sum(reach(other, up)[1] for other in range(span) if other != at)
        if total > 0:
            take(state0.at[:, :, pl.ds(0, total)], r_send.at[up])

    each_way(drain)
    for up, cond in ((1, has_up), (0, has_down)):
        pl.when(cond)(functools.partial(take, state2.at[:, :, pl.ds(0, PAD)], b_send.at[up]))

    others = stats.at[pl.ds(0, n - 1)]
    take(others, s_send)
    take(others, s_recv)
    total = stats[0]
    for k in range(1, n):
        total = total + stats[k]
    quotient = total / pltpu.roll(total, LANES // 2, 1)
    for c in range(chunks * groups):
        scal[pl.ds(c * SUB, SUB), :] = jnp.broadcast_to(quotient[:, c:c + 1], (SUB, LANES))

    def mixed(s, scale, o):
        at = pl.ds(s * lev * rows + o * SUB, SUB)
        return scale * flat_b[at, :] + out_ref[at, :]

    m0 = [mixed(0, scal[0:1, :], o) for o in range(pairs)]
    above = zero
    fades = [None] * pairs
    for o in range(pairs - 1, -1, -1):
        turn = flip(m0[o])
        col = above + 0.5 * m0[o] + jnp.where(low, turn, 0.0)
        fades[o] = jnp.exp((-0.5 / lev) * col)
        above = above + (m0[o] + turn)

    @pl.loop(0, chunks)
    def _(c):
        for i in range(chunk):
            s = c * chunk + i
            scale = scal[pl.ds(c * groups * SUB + i, 1), :]
            rate = rate_ref[s]
            for o in range(pairs):
                out_ref[pl.ds(s * lev * rows + o * SUB, SUB), :] = (
                    mixed(s, scale, o) * jnp.exp(-(rate * fades[o])))


def per_device(gx_n, halves, conc, winds, diffusivity, emission, photo_rate):
    spec, lev, rows, lanes = conc.shape
    span = lev // halves
    assert span * halves == lev and gx_n % span == 0 and lev % 2 == 0
    assert lanes == LANES and 2 * rows == SUB and span * rows == SUB and spec % 2 == 0
    n = gx_n * halves
    chunk = max(d for d in range(1, WIDTH + 1) if spec % d == 0)
    chunks = spec // chunk
    groups = -(-chunk // SUB)
    assert chunks * groups <= LANES // 2 and gx_n // span <= chunks + LAG_B
    deep = span * rows
    dims = (spec, lev, rows, halves, gx_n, span, chunk)
    f32 = jnp.float32
    hbm = pl.BlockSpec(memory_space=pl.ANY)
    dma = pltpu.SemaphoreType.DMA
    slots = (span + 2) * halves
    out = pl.pallas_call(
        functools.partial(kernel, dims),
        out_shape=pltpu.VMEM((spec * lev * rows, lanes), f32),
        in_specs=[hbm] * 5,
        out_specs=pl.BlockSpec(memory_space=pltpu.VMEM),
        scratch_shapes=[
            pltpu.SMEM((spec,), f32),
            pltpu.VMEM((lev - 1, rows, lanes), f32),
            pltpu.VMEM((spec * rows, lanes), f32),
            pltpu.VMEM((halves, spec, deep + 2 * SUB, lanes), f32),
            pltpu.VMEM((halves, chunk, 2 * SUB, lanes), f32),
            pltpu.VMEM((halves, spec, 2 * SUB, lanes), f32),
            pltpu.VMEM((halves, spec, deep, lanes), f32),
            pltpu.VMEM((spec, lev, rows, lanes), f32),
            pltpu.VMEM((slots, 2, rows, lanes), f32),
            pltpu.VMEM((2, halves, deep + 2 * SUB, lanes), f32),
            pltpu.VMEM((4, halves, 14, SUB, lanes), f32),
            pltpu.VMEM((2, groups * SUB * SUB, lanes), f32),
            pltpu.VMEM((SUB, lanes), f32),
            pltpu.VMEM((n, SUB, lanes), f32),
            pltpu.VMEM((chunks * groups * SUB, lanes), f32),
            dma((3,)),
            dma((3, lev)), dma((slots,)),
            dma((lev,)), dma((span, chunks)), dma(()),
            dma((2, halves)), dma((2,)), dma((2,)), dma((2, chunks)),
            dma((2,)), dma((2, chunks)),
            dma((lev,)), dma((chunks,)),
            dma(()), dma(()), pltpu.SemaphoreType.REGULAR((2,)),
        ],
        compiler_params=pltpu.CompilerParams(collective_id=0, has_side_effects=True),
    )(
        conc,
        winds,
        diffusivity,
        emission.reshape(spec * rows, lanes),
        photo_rate,
    )
    return out.reshape(spec, lev, rows, lanes)


def solution(mesh):
    halves = mesh.shape["gy"]
    gx_n = mesh.shape["gx"]
    return jax.shard_map(
        functools.partial(per_device, gx_n, halves),
        mesh=mesh,
        in_specs=(
            P(None, None, ("member", "gx"), "gy"),
            P(None, None, ("member", "gx"), "gy"),
            P(None, ("member", "gx"), "gy"),
            P(None, ("member", "gx"), "gy"),
            P(),
        ),
        out_specs=P(None, None, ("member", "gx"), "gy"),
        check_vma=False,
    )
```

```python
import functools

import jax
import jax.numpy as jnp
from jax import lax
from jax.experimental import pallas as pl
from jax.experimental.pallas import tpu as pltpu
from jax.sharding import PartitionSpec as P

BETAS = (1.0 / 3.0, 0.5, 1.0)
SUB = 8
LANES = 128
PAD = 3
WIDE = 2 * PAD
LAG_A = 5
LAG_B = 10
LAG_U = 15
WIDTH = 11
SLOT = LANES // SUB
MESH = pl.DeviceIdType.MESH


def stencil_weights(km, kp):
    def face(k):
        k = k / 60.0
        a = jnp.abs(k)
        return (
            k + a,
            -8.0 * k - 5.0 * a,
            37.0 * k + 10.0 * a,
            37.0 * k - 10.0 * a,
            -8.0 * k + 5.0 * a,
            k - a,
        )

    m, p = face(km), face(kp)
    return [-m[0]] + [p[j] - m[j + 1] for j in range(5)] + [p[5]]


def kernel(dims, conc_hbm, wind_hbm, diff_hbm, emis_hbm, rate_hbm, out_ref,
           rate_ref, diff_ref, emis_ref, state0, state1, state2, result, back,
           wrecv, cbuf, wts, part, stat, note, stats, scal,
           load_sem, w_send, w_recv, in_send, in_recv, own_recv, d_send, d_recv, r_send, a_recv,
           b_send, b_recv, out_send, out_recv, s_send, s_recv, token):
    spec, lev, rows, halves, gx_n, span, chunk = dims
    n = gx_n * halves
    chunks = spec // chunk
    groups = -(-chunk // SUB)
    deep = span * rows
    crews = gx_n // span
    slab, slab1, slab2 = deep + 2 * SUB, 2 * SUB, 2 * SUB
    my_gx, my_gy = lax.axis_index("gx"), lax.axis_index("gy")
    me = my_gx * halves + my_gy
    crew, seat = my_gx // span, my_gx % span
    my_lev = seat * halves + my_gy
    has_down, has_up = crew > 0, crew < crews - 1
    shift = span * halves

    def where_is(dev):
        return {"gx": dev // halves, "gy": dev % halves}

    def mate(at, half):
        return (crew * span + at) * halves + half

    barrier = pltpu.get_barrier_semaphore()

    def greet(dev):
        pl.semaphore_signal(barrier, inc=1, device_id=where_is(dev), device_id_type=MESH)

    for k in range(1, lev):
        m = (my_lev + k) % lev
        greet(mate(m // halves, m % halves))
    for cond, move in ((has_down, -shift), (has_up, shift)):
        @pl.when(cond)
        def _():
            for m in range(lev):
                greet(mate(m // halves, m % halves) + move)

    loads = [pltpu.make_async_copy(src, dst, load_sem.at[i]) for i, (src, dst) in enumerate(
        ((diff_hbm, diff_ref), (emis_hbm, emis_ref), (rate_hbm, rate_ref)))]
    for load in loads:
        load.start()

    def push(src, dst, dev, s_sem, r_sem):
        pltpu.make_async_remote_copy(
            src_ref=src, dst_ref=dst, send_sem=s_sem, recv_sem=r_sem,
            device_id=where_is(dev), device_id_type=MESH).start()

    def local(src, dst, r_sem):
        pltpu.make_async_copy(src, dst, r_sem).start()

    def take(like, sem):
        pltpu.make_async_copy(like, like, sem).wait()

    def group(c):
        return pl.ds(c * chunk, chunk)

    flat0 = state0.reshape(halves * spec * slab, LANES)
    flat1 = state1.reshape(halves * chunk * slab1, LANES)
    flat2 = state2.reshape(halves * spec * slab2, LANES)
    flat_r = result.reshape(halves * spec * deep, LANES)
    flat_b = back.reshape(spec * lev * rows, LANES)
    zero = jnp.zeros((SUB, LANES), jnp.float32)
    few = jnp.zeros((SUB // 2, LANES), jnp.float32)

    pl.semaphore_wait(barrier, lev - 1 + jnp.where(has_down, lev, 0) + jnp.where(has_up, lev, 0))

    own_rows = pl.ds(SUB + seat * rows, rows)

    def send_in(c):
        dst = state0.at[my_gy, group(c), own_rows]
        for k in range(1, span):
            at = (seat + k) % span
            for h in range(halves):
                push(conc_hbm.at[group(c), at * halves + h], dst, mate(at, h),
                     in_send.at[k * halves + h], in_recv.at[seat, c])

    def send_own():
        dst = state0.at[my_gy, :, own_rows]
        for k in range(1, halves):
            h = (my_gy + k) % halves
            push(conc_hbm.at[:, seat * halves + h], dst, mate(seat, h), in_send.at[k], own_recv)
        local(conc_hbm.at[:, my_lev], dst, own_recv)

    def reach(at, up):
        if up:
            first = max(0, deep - WIDE - at * rows)
            return first, rows - first, SUB - deep + at * rows + first
        return 0, max(0, min(rows, WIDE - at * rows)), SUB + deep + at * rows

    def each_way(act, landing=False):
        for up, cond in ((1, has_down if landing else has_up), (0, has_up if landing else has_down)):
            for at in range(span):
                pl.when(cond & (seat == at))(functools.partial(act, up, at))

    def send_direct():
        def act(up, at):
            first, count, land = reach(at, up)
            if count > 0:
                for h in range(halves):
                    push(conc_hbm.at[:, at * halves + h, pl.ds(first, count)],
                         state0.at[my_gy, :, pl.ds(land, count)],
                         mate(at, h) + (shift if up else -shift),
                         d_send.at[up, h], d_recv.at[up])

        each_way(act)

    def send_relay(c):
        def act(up, at):
            for other in range(span):
                first, count, land = reach(other, up)
                if other != at and count > 0:
                    push(state0.at[:, group(c), pl.ds(SUB + other * rows + first, count)],
                         state0.at[:, group(c), pl.ds(land, count)],
                         me + (shift if up else -shift), r_send.at[up], a_recv.at[up, c])

        each_way(act)

    sides = ((0, None, None), (1, has_up & (seat == span - 1), 0),
             (-1, has_down & (seat == 0), span + 1))

    def for_winds(act):
        for o, (step, cond, slot) in enumerate(sides):
            at = seat + 1 if slot is None else slot
            for lv in range(lev):
                dev = mate(lv // halves, lv % halves) + step * shift
                if cond is None:
                    pl.when(dev != me)(functools.partial(act, o, lv, dev, at))
                else:
                    pl.when(cond)(functools.partial(act, o, lv, dev, at))

    send_in(0)
    for_winds(lambda o, lv, dev, at: push(
        wind_hbm.at[:, lv], wrecv.at[at * halves + my_gy], dev, w_send.at[o, lv],
        w_recv.at[at * halves + my_gy]))
    local(wind_hbm.at[:, my_lev], wrecv.at[(seat + 1) * halves + my_gy],
          w_recv.at[(seat + 1) * halves + my_gy])

    send_own()

    @pl.loop(1, chunks)
    def _(c):
        send_in(c)

    send_direct()
    def clear(first0, first2):
        @pl.loop(0, halves * chunks)
        def _(i):
            for k in range(chunk):
                flat0[pl.ds((i * chunk + k) * slab + first0, SUB), :] = zero
                flat2[pl.ds((i * chunk + k) * slab2 + first2, SUB // 2), :] = few

    pl.when(crew == 0)(lambda: clear(0, 0))
    pl.when(crew == crews - 1)(lambda: clear(SUB + deep, SUB // 2 + deep))
    for h in range(halves):
        for c in range(2):
            cbuf[c, h, 0:SUB, :] = zero
            cbuf[c, h, SUB + deep:2 * SUB + deep, :] = zero
    part[...] = jnp.zeros_like(part)
    stat[...] = zero

    lane = lax.broadcasted_iota(jnp.int32, (SUB, LANES), 1)
    sub = lax.broadcasted_iota(jnp.int32, (SUB, LANES), 0)

    for load in loads:
        load.wait()
    ks = [diff_ref[lv] for lv in range(lev - 1)]
    none = jnp.zeros((rows, LANES), jnp.float32)
    lower, upper = [none] + ks, ks + [none]
    inv, ratio = [], []
    for lv in range(lev):
        pivot = 1.0 + lower[lv] + upper[lv]
        if lv:
            pivot = pivot - lower[lv] * ratio[-1]
        inv.append(1.0 / pivot)
        ratio.append(upper[lv] * inv[lv])
    inverse = [[None] * lev for _ in range(lev)]
    for j in range(lev):
        val = [none] * lev
        for lv in range(j, lev):
            val[lv] = inv[lv] if lv == j else lower[lv] * val[lv - 1] * inv[lv]
        for lv in range(lev - 1, -1, -1):
            inverse[lv][j] = val[lv] if lv == lev - 1 else val[lv] + ratio[lv] * inverse[lv + 1][j]
    pairs = lev // 2

    def duo(a, b):
        return jnp.concatenate([a, b], axis=0)

    mats = [[(duo(inverse[2 * o][2 * i], inverse[2 * o + 1][2 * i + 1]),
              duo(inverse[2 * o][2 * i + 1], inverse[2 * o + 1][2 * i]))
             for i in range(pairs)] for o in range(pairs)]
    first_col = [duo(inverse[2 * o][0], inverse[2 * o + 1][0]) for o in range(pairs)]

    def flip(v):
        return pltpu.roll(v, SUB // 2, 0)

    low = sub < SUB // 2

    @pl.loop(0, spec // 2)
    def _(s):
        e = emis_ref[pl.ds(s * SUB, SUB), :]
        f = flip(e)
        for k, v in enumerate((jnp.where(low, e, f), jnp.where(low, f, e))):
            for o in range(pairs):
                out_ref[pl.ds((2 * s + k) * lev * rows + o * SUB, SUB), :] = first_col[o] * v

    def wind_in(slot):
        for h in range(halves):
            take(wrecv.at[slot * halves + h], w_recv.at[slot * halves + h])
            for c in range(2):
                base = SUB + (slot - 1) * rows
                cbuf[c, h, base:base + rows, :] = wrecv[slot * halves + h, c]

    for slot in range(1, span + 1):
        wind_in(slot)
    pl.when(has_down)(lambda: wind_in(0))
    pl.when(has_up)(lambda: wind_in(span + 1))

    passes = ((0, -PAD), (0, deep - SUB + PAD), (1, 0), (2, 0))
    for q, (s, r0) in enumerate(passes):
        at_row = crew * deep + r0 + sub
        inside = (at_row >= 0) & (at_row < crews * deep)
        for h in range(halves):
            here, left, right = (cbuf[0, h, SUB + r0 + d:2 * SUB + r0 + d, :] for d in (0, -1, 1))
            for j, w in enumerate(stencil_weights(0.5 * (left + here), 0.5 * (here + right))):
                wts[q, h, j] = jnp.where(inside, w, 0.0) * BETAS[s]
        cy = [cbuf[1, h, SUB + r0:2 * SUB + r0, :] for h in range(halves)]
        for h in range(halves):
            nxt = pltpu.roll(cy[h + 1], LANES - 1, 1) if h + 1 < halves else zero
            prv = pltpu.roll(cy[h - 1], 1, 1) if h > 0 else zero
            up = jnp.where(lane < LANES - 1, pltpu.roll(cy[h], LANES - 1, 1), nxt)
            down = jnp.where(lane >= 1, pltpu.roll(cy[h], 1, 1), prv)
            ws = stencil_weights(0.5 * (down + cy[h]), 0.5 * (cy[h] + up))
            for j, w in enumerate(ws):
                d = j - 3
                if d > 0 and h == halves - 1:
                    w = jnp.where(lane < LANES - d, w, 0.0)
                if d < 0 and h == 0:
                    w = jnp.where(lane >= -d, w, 0.0)
                wts[q, h, 7 + j] = w * BETAS[s]

    def step(q, count, src, src_at, start, start_at, put):
        wx = [[wts[q, h, j] for j in range(7)] for h in range(halves)]
        wy = [[wts[q, h, 7 + j] for j in range(7)] for h in range(halves)]
        for i in range(count):
            partial, new = [], []
            for h in range(halves):
                base = src_at(h, i)
                mid = None
                acc = None
                for j in range(7):
                    v = src[pl.ds(base + j, SUB), :]
                    if j == PAD:
                        mid = v
                    acc = wx[h][j] * v if acc is None else acc + wx[h][j] * v
                p = mid - acc
                partial.append(p)
                begin = mid if start is None else start[pl.ds(start_at(h, i), SUB), :]
                new.append(begin - acc - wy[h][3] * p)
            for d in (1, 2, 3):
                up = [pltpu.roll(p, LANES - d, 1) for p in partial]
                down = [pltpu.roll(p, d, 1) for p in partial]
                for h in range(halves):
                    u = up[h] if h == halves - 1 else jnp.where(lane < LANES - d, up[h], up[h + 1])
                    w = down[h] if h == 0 else jnp.where(lane >= d, down[h], down[h - 1])
                    new[h] = new[h] - (wy[h][3 + d] * u + wy[h][3 - d] * w)
            put(i, new)

    def at0(c):
        return lambda h, i: (h * spec + c * chunk + i) * slab

    def send_edge(c):
        for up, cond in ((1, has_up), (0, has_down)):
            first = SUB // 2 + (deep - PAD if up else 0)
            land = SUB // 2 + (-PAD if up else deep)
            pl.when(cond)(functools.partial(
                push, state2.at[:, group(c), pl.ds(first, PAD)],
                state2.at[:, group(c), pl.ds(land, PAD)],
                me + (shift if up else -shift), b_send.at[up], b_recv.at[up, c]))

    def arrive(up, at):
        count = reach(at, up)[1]
        if count > 0:
            take(state0.at[:, :, pl.ds(0, count)], d_recv.at[up])

    def arrive_relay(c, up, at):
        total = sum(reach(other, up)[1] for other in range(span) if other != at)
        if total > 0:
            take(state0.at[:, group(c), pl.ds(0, total)], a_recv.at[up, c])

    def early(c):

        @pl.when(c == 0)
        def _():
            take(state0.at[:, :, pl.ds(0, rows)], own_recv)
            each_way(arrive, True)

        each_way(functools.partial(arrive_relay, c), True)
        base = at0(c)
        for q in (0, 1):
            off = passes[q][1]

            def put(i, new, off=off):
                for h in range(halves):
                    flat1[pl.ds((h * chunk + i) * slab1 + off + PAD, SUB), :] = new[h]

            step(q, chunk, flat0, lambda h, i: base(h, i) + SUB + off - PAD, None, None, put)

        def put(i, new):
            for h in range(halves):
                flat2[pl.ds((h * spec + c * chunk + i) * slab2 + SUB // 2, SUB), :] = new[h]

        step(2, chunk, flat1, lambda h, i: (h * chunk + i) * slab1, flat0,
             lambda h, i: base(h, i) + SUB, put)
        send_edge(c)

    def late(c):
        pl.when(has_down)(lambda: take(state2.at[:, group(c), pl.ds(0, PAD)], b_recv.at[1, c]))
        pl.when(has_up)(lambda: take(state2.at[:, group(c), pl.ds(0, PAD)], b_recv.at[0, c]))
        base = at0(c)

        def put(i, new):
            net, pos = None, None
            for h in range(halves):
                flat_r[pl.ds((h * spec + c * chunk + i) * deep, SUB), :] = new[h]
                p = jnp.maximum(new[h], 0.0)
                net, pos = (new[h], p) if net is None else (net + new[h], pos + p)
            part[0, pl.ds(i * SUB, SUB), :] = net
            part[1, pl.ds(i * SUB, SUB), :] = pos

        step(3, chunk, flat2, lambda h, i: (h * spec + c * chunk + i) * slab2 + SUB // 2 - PAD,
             flat0, lambda h, i: base(h, i) + SUB, put)
        acc = stat[...]
        for o in range(2):
            for g in range(groups):
                first = g * SUB * SUB
                tot = part[o, pl.ds(first, SUB, stride=SUB), :]
                for r in range(1, SUB):
                    tot = tot + part[o, pl.ds(first + r, SUB, stride=SUB), :]
                acc = jnp.where(lane == c * groups + g + o * (LANES // 2),
                                jnp.sum(tot, axis=1, keepdims=True), acc)
        stat[...] = acc

        @pl.when(c == chunks - 1)
        def _():
            def send_stat(k, carry):
                dev = (k + me) % n
                push(note, stats.at[me], dev, s_send, s_recv)
                return carry

            rows_of = []
            for o in range(2):
                mine = jnp.where(lane < SLOT, pltpu.roll(acc, o * (LANES // 2), 1), 0.0)
                spread = pltpu.roll(mine, 0, 1, stride=SLOT, stride_axis=0)
                rows_of.append(jnp.sum(spread, axis=0, keepdims=True))
            packed = jnp.concatenate(rows_of, axis=0)
            note[...] = packed
            lax.fori_loop(1, n, send_stat, 0)
            stats[pl.ds(me, 1)] = packed[None]

        for k in range(1, span * halves):
            m = (my_lev + k) % (span * halves)
            push(result.at[m % halves, group(c), pl.ds((m // halves) * rows, rows)],
                 back.at[group(c), my_lev], mate(m // halves, m % halves),
                 out_send.at[k], out_recv.at[c])
        local(result.at[my_gy, group(c), pl.ds(seat * rows, rows)],
              back.at[group(c), my_lev], out_recv.at[c])

    def solve(c):
        take(back.at[group(c)], out_recv.at[c])
        for i in range(chunk):
            base = (c * chunk + i) * lev * rows
            tiles = [jnp.maximum(flat_b[pl.ds(base + o * SUB, SUB), :], 0.0) for o in range(pairs)]
            swaps = [flip(t) for t in tiles]
            for o in range(pairs):
                acc = None
                for k in range(pairs):
                    term = mats[o][k][0] * tiles[k] + mats[o][k][1] * swaps[k]
                    acc = term if acc is None else acc + term
                flat_b[pl.ds(base + o * SUB, SUB), :] = acc

    def pass_on(up):
        pl.semaphore_signal(token.at[up], inc=1, device_id=where_is(me + (shift if up else -shift)),
                            device_id_type=MESH)

    pl.when(has_up & (crew == 0))(lambda: pass_on(1))
    pl.when(has_down & (crew == crews - 1))(lambda: pass_on(0))

    @pl.loop(0, chunks + LAG_U)
    def _(i):
        for up, cond, on, turn in ((1, has_down, has_up, crew), (0, has_up, has_down, crews - 1 - crew)):
            @pl.when(cond & (i == turn))
            def _():
                pl.semaphore_wait(token.at[up], 1)
                pl.when(on)(functools.partial(pass_on, up))

        @pl.when(i < chunks)
        def _():
            for k in range(1, span):
                at = (seat + k) % span
                take(state0.at[:, group(i), pl.ds(0, rows)], in_recv.at[at, i])
            send_relay(i)

        @pl.when((i >= LAG_A) & (i < LAG_A + chunks))
        def _():
            early(i - LAG_A)

        @pl.when((i >= LAG_B) & (i < LAG_B + chunks))
        def _():
            late(i - LAG_B)

        @pl.when(i >= LAG_U)
        def _():
            solve(i - LAG_U)

    for_winds(lambda o, lv, dev, at: take(wrecv.at[0], w_send.at[o, lv]))
    whole = state0.at[0, :, pl.ds(0, rows)]
    for k in range(1, span * halves):
        take(whole, in_send.at[k])
        take(whole, out_send.at[k])

    def drain(up, at):
        _, count, _ = reach(at, up)
        if count > 0:
            for h in range(halves):
                take(state0.at[0, :, pl.ds(0, count)], d_send.at[up, h])
        total = sum(reach(other, up)[1] for other in range(span) if other != at)
        if total > 0:
            take(state0.at[:, :, pl.ds(0, total)], r_send.at[up])

    each_way(drain)
    for up, cond in ((1, has_up), (0, has_down)):
        pl.when(cond)(functools.partial(take, state2.at[:, :, pl.ds(0, PAD)], b_send.at[up]))

    others = stats.at[pl.ds(0, n - 1)]
    take(others, s_send)
    take(others, s_recv)
    total = stats[0]
    for k in range(1, n):
        total = total + stats[k]
    line = jnp.broadcast_to(total[0:1] / total[1:2], (SUB, LANES))
    quotient = line
    for k in range(1, SUB):
        quotient = jnp.where(sub == k, pltpu.roll(line, LANES - k * SLOT, 1), quotient)
    for c in range(chunks * groups):
        scal[pl.ds(c * SUB, SUB), :] = jnp.broadcast_to(quotient[:, c:c + 1], (SUB, LANES))

    def mixed(s, scale, o):
        at = pl.ds(s * lev * rows + o * SUB, SUB)
        return scale * flat_b[at, :] + out_ref[at, :]

    m0 = [mixed(0, scal[0:1, :], o) for o in range(pairs)]
    above = zero
    fades = [None] * pairs
    for o in range(pairs - 1, -1, -1):
        turn = flip(m0[o])
        col = above + 0.5 * m0[o] + jnp.where(low, turn, 0.0)
        fades[o] = jnp.exp((-0.5 / lev) * col)
        above = above + (m0[o] + turn)

    @pl.loop(0, chunks)
    def _(c):
        for i in range(chunk):
            s = c * chunk + i
            scale = scal[pl.ds(c * groups * SUB + i, 1), :]
            rate = rate_ref[s]
            for o in range(pairs):
                out_ref[pl.ds(s * lev * rows + o * SUB, SUB), :] = (
                    mixed(s, scale, o) * jnp.exp(-(rate * fades[o])))


def per_device(gx_n, halves, conc, winds, diffusivity, emission, photo_rate):
    spec, lev, rows, lanes = conc.shape
    span = lev // halves
    assert span * halves == lev and gx_n % span == 0 and lev % 2 == 0
    assert lanes == LANES and 2 * rows == SUB and span * rows == SUB and spec % 2 == 0
    n = gx_n * halves
    chunk = max(d for d in range(1, WIDTH + 1) if spec % d == 0)
    chunks = spec // chunk
    groups = -(-chunk // SUB)
    assert chunks * groups <= SLOT and gx_n // span <= chunks + LAG_B
    deep = span * rows
    dims = (spec, lev, rows, halves, gx_n, span, chunk)
    f32 = jnp.float32
    hbm = pl.BlockSpec(memory_space=pl.ANY)
    dma = pltpu.SemaphoreType.DMA
    slots = (span + 2) * halves
    out = pl.pallas_call(
        functools.partial(kernel, dims),
        out_shape=pltpu.VMEM((spec * lev * rows, lanes), f32),
        in_specs=[hbm] * 5,
        out_specs=pl.BlockSpec(memory_space=pltpu.VMEM),
        scratch_shapes=[
            pltpu.SMEM((spec,), f32),
            pltpu.VMEM((lev - 1, rows, lanes), f32),
            pltpu.VMEM((spec * rows, lanes), f32),
            pltpu.VMEM((halves, spec, deep + 2 * SUB, lanes), f32),
            pltpu.VMEM((halves, chunk, 2 * SUB, lanes), f32),
            pltpu.VMEM((halves, spec, 2 * SUB, lanes), f32),
            pltpu.VMEM((halves, spec, deep, lanes), f32),
            pltpu.VMEM((spec, lev, rows, lanes), f32),
            pltpu.VMEM((slots, 2, rows, lanes), f32),
            pltpu.VMEM((2, halves, deep + 2 * SUB, lanes), f32),
            pltpu.VMEM((4, halves, 14, SUB, lanes), f32),
            pltpu.VMEM((2, groups * SUB * SUB, lanes), f32),
            pltpu.VMEM((SUB, lanes), f32),
            pltpu.VMEM((2, lanes), f32),
            pltpu.VMEM((n, 2, lanes), f32),
            pltpu.VMEM((chunks * groups * SUB, lanes), f32),
            dma((3,)),
            dma((3, lev)), dma((slots,)),
            dma((lev,)), dma((span, chunks)), dma(()),
            dma((2, halves)), dma((2,)), dma((2,)), dma((2, chunks)),
            dma((2,)), dma((2, chunks)),
            dma((lev,)), dma((chunks,)),
            dma(()), dma(()), pltpu.SemaphoreType.REGULAR((2,)),
        ],
        compiler_params=pltpu.CompilerParams(collective_id=0, has_side_effects=True),
    )(
        conc,
        winds,
        diffusivity,
        emission.reshape(spec * rows, lanes),
        photo_rate,
    )
    return out.reshape(spec, lev, rows, lanes)


def solution(mesh):
    halves = mesh.shape["gy"]
    gx_n = mesh.shape["gx"]
    return jax.shard_map(
        functools.partial(per_device, gx_n, halves),
        mesh=mesh,
        in_specs=(
            P(None, None, ("member", "gx"), "gy"),
            P(None, None, ("member", "gx"), "gy"),
            P(None, ("member", "gx"), "gy"),
            P(None, ("member", "gx"), "gy"),
            P(),
        ),
        out_specs=P(None, None, ("member", "gx"), "gy"),
        check_vma=False,
    )
```

```python
import functools

import jax
import jax.numpy as jnp
from jax import lax
from jax.experimental import pallas as pl
from jax.experimental.pallas import tpu as pltpu
from jax.sharding import PartitionSpec as P

BETAS = (1.0 / 3.0, 0.5, 1.0)
SUB = 8
LANES = 128
PAD = 3
WIDE = 2 * PAD
LAG_A = 6
LAG_B = 11
LAG_U = 16
WIDTH = 11
SLOT = LANES // SUB
MESH = pl.DeviceIdType.MESH


def stencil_weights(km, kp):
    def face(k):
        k = k / 60.0
        a = jnp.abs(k)
        return (
            k + a,
            -8.0 * k - 5.0 * a,
            37.0 * k + 10.0 * a,
            37.0 * k - 10.0 * a,
            -8.0 * k + 5.0 * a,
            k - a,
        )

    m, p = face(km), face(kp)
    return [-m[0]] + [p[j] - m[j + 1] for j in range(5)] + [p[5]]


def kernel(dims, conc_hbm, wind_hbm, diff_hbm, emis_hbm, rate_hbm, out_ref,
           rate_ref, diff_ref, emis_ref, state0, state1, state2, result, back,
           wrecv, cbuf, wts, part, stat, note, stats, scal,
           load_sem, w_send, w_recv, in_send, in_recv, own_recv, d_send, d_recv, r_send, a_recv,
           b_send, b_recv, out_send, out_recv, s_send, s_recv, token):
    spec, lev, rows, halves, gx_n, span, chunk = dims
    n = gx_n * halves
    chunks = spec // chunk
    groups = -(-chunk // SUB)
    deep = span * rows
    crews = gx_n // span
    slab, slab1, slab2 = deep + 2 * SUB, 2 * SUB, 2 * SUB
    my_gx, my_gy = lax.axis_index("gx"), lax.axis_index("gy")
    me = my_gx * halves + my_gy
    crew, seat = my_gx // span, my_gx % span
    my_lev = seat * halves + my_gy
    has_down, has_up = crew > 0, crew < crews - 1
    shift = span * halves

    def where_is(dev):
        return {"gx": dev // halves, "gy": dev % halves}

    def mate(at, half):
        return (crew * span + at) * halves + half

    barrier = pltpu.get_barrier_semaphore()

    def greet(dev):
        pl.semaphore_signal(barrier, inc=1, device_id=where_is(dev), device_id_type=MESH)

    for k in range(1, lev):
        m = (my_lev + k) % lev
        greet(mate(m // halves, m % halves))
    for cond, move in ((has_down, -shift), (has_up, shift)):
        @pl.when(cond)
        def _():
            for h in range(halves):
                greet(mate(seat, h) + move)

    loads = [pltpu.make_async_copy(src, dst, load_sem.at[i]) for i, (src, dst) in enumerate(
        ((diff_hbm, diff_ref), (emis_hbm, emis_ref), (rate_hbm, rate_ref)))]
    for load in loads:
        load.start()

    def push(src, dst, dev, s_sem, r_sem):
        pltpu.make_async_remote_copy(
            src_ref=src, dst_ref=dst, send_sem=s_sem, recv_sem=r_sem,
            device_id=where_is(dev), device_id_type=MESH).start()

    def local(src, dst, r_sem):
        pltpu.make_async_copy(src, dst, r_sem).start()

    def take(like, sem):
        pltpu.make_async_copy(like, like, sem).wait()

    def group(c):
        return pl.ds(c * chunk, chunk)

    flat0 = state0.reshape(halves * spec * slab, LANES)
    flat1 = state1.reshape(halves * chunk * slab1, LANES)
    flat2 = state2.reshape(halves * spec * slab2, LANES)
    flat_r = result.reshape(halves * spec * deep, LANES)
    flat_b = back.reshape(spec * lev * rows, LANES)
    zero = jnp.zeros((SUB, LANES), jnp.float32)
    few = jnp.zeros((SUB // 2, LANES), jnp.float32)

    pl.semaphore_wait(barrier, lev - 1 + jnp.where(has_down, halves, 0) + jnp.where(has_up, halves, 0))

    own_rows = pl.ds(SUB + seat * rows, rows)

    def send_in(c):
        dst = state0.at[my_gy, group(c), own_rows]
        for k in range(1, span):
            at = (seat + k) % span
            for h in range(halves):
                push(conc_hbm.at[group(c), at * halves + h], dst, mate(at, h),
                     in_send.at[k * halves + h], in_recv.at[seat, c])

    def send_own():
        dst = state0.at[my_gy, :, own_rows]
        for k in range(1, halves):
            h = (my_gy + k) % halves
            push(conc_hbm.at[:, seat * halves + h], dst, mate(seat, h), in_send.at[k], own_recv)
        local(conc_hbm.at[:, my_lev], dst, own_recv)

    def reach(at, up):
        if up:
            first = max(0, deep - WIDE - at * rows)
            return first, rows - first, SUB - deep + at * rows + first
        return 0, max(0, min(rows, WIDE - at * rows)), SUB + deep + at * rows

    def each_way(act, landing=False):
        for up, cond in ((1, has_down if landing else has_up), (0, has_up if landing else has_down)):
            for at in range(span):
                pl.when(cond & (seat == at))(functools.partial(act, up, at))

    def send_direct():
        def act(up, at):
            first, count, land = reach(at, up)
            if count > 0:
                for h in range(halves):
                    push(conc_hbm.at[:, at * halves + h, pl.ds(first, count)],
                         state0.at[my_gy, :, pl.ds(land, count)],
                         mate(at, h) + (shift if up else -shift),
                         d_send.at[up, h], d_recv.at[up])

        each_way(act)

    def send_relay(c):
        def act(up, at):
            for other in range(span):
                first, count, land = reach(other, up)
                if other != at and count > 0:
                    push(state0.at[:, group(c), pl.ds(SUB + other * rows + first, count)],
                         state0.at[:, group(c), pl.ds(land, count)],
                         me + (shift if up else -shift), r_send.at[up], a_recv.at[up, c])

        each_way(act)

    edges = ((1, has_up, span - 1, 0), (0, has_down, 0, span + 1))

    def send_winds():
        for k in range(1, lev):
            m = (my_lev + k) % lev
            push(wind_hbm.at[:, m], wrecv.at[(seat + 1) * halves + my_gy], mate(m // halves, m % halves),
                 w_send.at[2, k], w_recv.at[(seat + 1) * halves + my_gy])
        local(wind_hbm.at[:, my_lev], wrecv.at[(seat + 1) * halves + my_gy],
              w_recv.at[(seat + 1) * halves + my_gy])
        for up, cond, edge, slot in edges:
            @pl.when(cond & (seat == edge))
            def _():
                for h in range(halves):
                    push(wind_hbm.at[:, edge * halves + h], wrecv.at[slot * halves + my_gy],
                         mate(edge, h) + (shift if up else -shift),
                         w_send.at[up, h], w_recv.at[slot * halves + my_gy])

    def relay_winds():
        for at in range(span):
            for h in range(halves):
                k = (at + 1) * halves + h
                take(wrecv.at[k], w_recv.at[k])
        for up, cond, edge, slot in edges:
            @pl.when(cond & (seat != edge))
            def _():
                for h in range(halves):
                    push(wrecv.at[(edge + 1) * halves + h], wrecv.at[slot * halves + h],
                         me + (shift if up else -shift),
                         w_send.at[up, h], w_recv.at[slot * halves + h])

    send_winds()
    send_in(0)
    send_own()

    @pl.loop(1, chunks)
    def _(c):
        send_in(c)

    send_direct()
    def clear(first0, first2):
        @pl.loop(0, halves * chunks)
        def _(i):
            for k in range(chunk):
                flat0[pl.ds((i * chunk + k) * slab + first0, SUB), :] = zero
                flat2[pl.ds((i * chunk + k) * slab2 + first2, SUB // 2), :] = few

    pl.when(crew == 0)(lambda: clear(0, 0))
    pl.when(crew == crews - 1)(lambda: clear(SUB + deep, SUB // 2 + deep))
    for h in range(halves):
        for c in range(2):
            cbuf[c, h, 0:SUB, :] = zero
            cbuf[c, h, SUB + deep:2 * SUB + deep, :] = zero
    part[...] = jnp.zeros_like(part)
    stat[...] = zero

    lane = lax.broadcasted_iota(jnp.int32, (SUB, LANES), 1)
    sub = lax.broadcasted_iota(jnp.int32, (SUB, LANES), 0)

    for load in loads:
        load.wait()
    ks = [diff_ref[lv] for lv in range(lev - 1)]
    none = jnp.zeros((rows, LANES), jnp.float32)
    lower, upper = [none] + ks, ks + [none]
    inv, ratio = [], []
    for lv in range(lev):
        pivot = 1.0 + lower[lv] + upper[lv]
        if lv:
            pivot = pivot - lower[lv] * ratio[-1]
        inv.append(1.0 / pivot)
        ratio.append(upper[lv] * inv[lv])
    inverse = [[None] * lev for _ in range(lev)]
    for j in range(lev):
        val = [none] * lev
        for lv in range(j, lev):
            val[lv] = inv[lv] if lv == j else lower[lv] * val[lv - 1] * inv[lv]
        for lv in range(lev - 1, -1, -1):
            inverse[lv][j] = val[lv] if lv == lev - 1 else val[lv] + ratio[lv] * inverse[lv + 1][j]
    pairs = lev // 2

    def duo(a, b):
        return jnp.concatenate([a, b], axis=0)

    mats = [[(duo(inverse[2 * o][2 * i], inverse[2 * o + 1][2 * i + 1]),
              duo(inverse[2 * o][2 * i + 1], inverse[2 * o + 1][2 * i]))
             for i in range(pairs)] for o in range(pairs)]
    first_col = [duo(inverse[2 * o][0], inverse[2 * o + 1][0]) for o in range(pairs)]

    def flip(v):
        return pltpu.roll(v, SUB // 2, 0)

    low = sub < SUB // 2

    @pl.loop(0, spec // 2)
    def _(s):
        e = emis_ref[pl.ds(s * SUB, SUB), :]
        f = flip(e)
        for k, v in enumerate((jnp.where(low, e, f), jnp.where(low, f, e))):
            for o in range(pairs):
                out_ref[pl.ds((2 * s + k) * lev * rows + o * SUB, SUB), :] = first_col[o] * v

    relay_winds()

    passes = ((0, -PAD), (0, deep - SUB + PAD), (1, 0), (2, 0))

    def weigh():
        def wind_in(slot, wait=True):
            for h in range(halves):
                if wait:
                    take(wrecv.at[slot * halves + h], w_recv.at[slot * halves + h])
                for c in range(2):
                    base = SUB + (slot - 1) * rows
                    cbuf[c, h, base:base + rows, :] = wrecv[slot * halves + h, c]

        for slot in range(1, span + 1):
            wind_in(slot, False)
        pl.when(has_down)(lambda: wind_in(0))
        pl.when(has_up)(lambda: wind_in(span + 1))

        for q, (s, r0) in enumerate(passes):
            at_row = crew * deep + r0 + sub
            inside = (at_row >= 0) & (at_row < crews * deep)
            for h in range(halves):
                here, left, right = (cbuf[0, h, SUB + r0 + d:2 * SUB + r0 + d, :] for d in (0, -1, 1))
                for j, w in enumerate(stencil_weights(0.5 * (left + here), 0.5 * (here + right))):
                    wts[q, h, j] = jnp.where(inside, w, 0.0) * BETAS[s]
            cy = [cbuf[1, h, SUB + r0:2 * SUB + r0, :] for h in range(halves)]
            for h in range(halves):
                nxt = pltpu.roll(cy[h + 1], LANES - 1, 1) if h + 1 < halves else zero
                prv = pltpu.roll(cy[h - 1], 1, 1) if h > 0 else zero
                up = jnp.where(lane < LANES - 1, pltpu.roll(cy[h], LANES - 1, 1), nxt)
                down = jnp.where(lane >= 1, pltpu.roll(cy[h], 1, 1), prv)
                ws = stencil_weights(0.5 * (down + cy[h]), 0.5 * (cy[h] + up))
                for j, w in enumerate(ws):
                    d = j - 3
                    if d > 0 and h == halves - 1:
                        w = jnp.where(lane < LANES - d, w, 0.0)
                    if d < 0 and h == 0:
                        w = jnp.where(lane >= -d, w, 0.0)
                    wts[q, h, 7 + j] = w * BETAS[s]

    def step(q, count, src, src_at, start, start_at, put):
        wx = [[wts[q, h, j] for j in range(7)] for h in range(halves)]
        wy = [[wts[q, h, 7 + j] for j in range(7)] for h in range(halves)]
        for i in range(count):
            partial, new = [], []
            for h in range(halves):
                base = src_at(h, i)
                mid = None
                acc = None
                for j in range(7):
                    v = src[pl.ds(base + j, SUB), :]
                    if j == PAD:
                        mid = v
                    acc = wx[h][j] * v if acc is None else acc + wx[h][j] * v
                p = mid - acc
                partial.append(p)
                begin = mid if start is None else start[pl.ds(start_at(h, i), SUB), :]
                new.append(begin - acc - wy[h][3] * p)
            for d in (1, 2, 3):
                up = [pltpu.roll(p, LANES - d, 1) for p in partial]
                down = [pltpu.roll(p, d, 1) for p in partial]
                for h in range(halves):
                    u = up[h] if h == halves - 1 else jnp.where(lane < LANES - d, up[h], up[h + 1])
                    w = down[h] if h == 0 else jnp.where(lane >= d, down[h], down[h - 1])
                    new[h] = new[h] - (wy[h][3 + d] * u + wy[h][3 - d] * w)
            put(i, new)

    def at0(c):
        return lambda h, i: (h * spec + c * chunk + i) * slab

    def send_edge(c):
        for up, cond in ((1, has_up), (0, has_down)):
            first = SUB // 2 + (deep - PAD if up else 0)
            land = SUB // 2 + (-PAD if up else deep)
            pl.when(cond)(functools.partial(
                push, state2.at[:, group(c), pl.ds(first, PAD)],
                state2.at[:, group(c), pl.ds(land, PAD)],
                me + (shift if up else -shift), b_send.at[up], b_recv.at[up, c]))

    def arrive(up, at):
        count = reach(at, up)[1]
        if count > 0:
            take(state0.at[:, :, pl.ds(0, count)], d_recv.at[up])

    def arrive_relay(c, up, at):
        total = sum(reach(other, up)[1] for other in range(span) if other != at)
        if total > 0:
            take(state0.at[:, group(c), pl.ds(0, total)], a_recv.at[up, c])

    def early(c):

        @pl.when(c == 0)
        def _():
            take(state0.at[:, :, pl.ds(0, rows)], own_recv)
            each_way(arrive, True)

        each_way(functools.partial(arrive_relay, c), True)
        base = at0(c)
        for q in (0, 1):
            off = passes[q][1]

            def put(i, new, off=off):
                for h in range(halves):
                    flat1[pl.ds((h * chunk + i) * slab1 + off + PAD, SUB), :] = new[h]

            step(q, chunk, flat0, lambda h, i: base(h, i) + SUB + off - PAD, None, None, put)

        def put(i, new):
            for h in range(halves):
                flat2[pl.ds((h * spec + c * chunk + i) * slab2 + SUB // 2, SUB), :] = new[h]

        step(2, chunk, flat1, lambda h, i: (h * chunk + i) * slab1, flat0,
             lambda h, i: base(h, i) + SUB, put)
        send_edge(c)

    def late(c):
        pl.when(has_down)(lambda: take(state2.at[:, group(c), pl.ds(0, PAD)], b_recv.at[1, c]))
        pl.when(has_up)(lambda: take(state2.at[:, group(c), pl.ds(0, PAD)], b_recv.at[0, c]))
        base = at0(c)

        def put(i, new):
            net, pos = None, None
            for h in range(halves):
                flat_r[pl.ds((h * spec + c * chunk + i) * deep, SUB), :] = new[h]
                p = jnp.maximum(new[h], 0.0)
                net, pos = (new[h], p) if net is None else (net + new[h], pos + p)
            part[0, pl.ds(i * SUB, SUB), :] = net
            part[1, pl.ds(i * SUB, SUB), :] = pos

        step(3, chunk, flat2, lambda h, i: (h * spec + c * chunk + i) * slab2 + SUB // 2 - PAD,
             flat0, lambda h, i: base(h, i) + SUB, put)
        acc = stat[...]
        for o in range(2):
            for g in range(groups):
                first = g * SUB * SUB
                tot = part[o, pl.ds(first, SUB, stride=SUB), :]
                for r in range(1, SUB):
                    tot = tot + part[o, pl.ds(first + r, SUB, stride=SUB), :]
                acc = jnp.where(lane == c * groups + g + o * (LANES // 2),
                                jnp.sum(tot, axis=1, keepdims=True), acc)
        stat[...] = acc

        @pl.when(c == chunks - 1)
        def _():
            def send_stat(k, carry):
                dev = (k + me) % n
                push(note, stats.at[me], dev, s_send, s_recv)
                return carry

            rows_of = []
            for o in range(2):
                mine = jnp.where(lane < SLOT, pltpu.roll(acc, o * (LANES // 2), 1), 0.0)
                spread = pltpu.roll(mine, 0, 1, stride=SLOT, stride_axis=0)
                rows_of.append(jnp.sum(spread, axis=0, keepdims=True))
            packed = jnp.concatenate(rows_of, axis=0)
            note[...] = packed
            lax.fori_loop(1, n, send_stat, 0)
            stats[pl.ds(me, 1)] = packed[None]

        for k in range(1, span * halves):
            m = (my_lev + k) % (span * halves)
            push(result.at[m % halves, group(c), pl.ds((m // halves) * rows, rows)],
                 back.at[group(c), my_lev], mate(m // halves, m % halves),
                 out_send.at[k], out_recv.at[c])
        local(result.at[my_gy, group(c), pl.ds(seat * rows, rows)],
              back.at[group(c), my_lev], out_recv.at[c])

    def solve(c):
        take(back.at[group(c)], out_recv.at[c])
        for i in range(chunk):
            base = (c * chunk + i) * lev * rows
            tiles = [jnp.maximum(flat_b[pl.ds(base + o * SUB, SUB), :], 0.0) for o in range(pairs)]
            swaps = [flip(t) for t in tiles]
            for o in range(pairs):
                acc = None
                for k in range(pairs):
                    term = mats[o][k][0] * tiles[k] + mats[o][k][1] * swaps[k]
                    acc = term if acc is None else acc + term
                flat_b[pl.ds(base + o * SUB, SUB), :] = acc

    def pass_on(up):
        pl.semaphore_signal(token.at[up], inc=1, device_id=where_is(me + (shift if up else -shift)),
                            device_id_type=MESH)

    pl.when(has_up & (crew == 0))(lambda: pass_on(1))
    pl.when(has_down & (crew == crews - 1))(lambda: pass_on(0))

    @pl.loop(0, chunks + LAG_U)
    def _(i):
        for up, cond, on, turn in ((1, has_down, has_up, crew), (0, has_up, has_down, crews - 1 - crew)):
            @pl.when(cond & (i == turn))
            def _():
                pl.semaphore_wait(token.at[up], 1)
                pl.when(on)(functools.partial(pass_on, up))

        @pl.when(i < chunks)
        def _():
            for k in range(1, span):
                at = (seat + k) % span
                take(state0.at[:, group(i), pl.ds(0, rows)], in_recv.at[at, i])
            send_relay(i)

        pl.when(i == LAG_A)(weigh)

        @pl.when((i >= LAG_A) & (i < LAG_A + chunks))
        def _():
            early(i - LAG_A)

        @pl.when((i >= LAG_B) & (i < LAG_B + chunks))
        def _():
            late(i - LAG_B)

        @pl.when(i >= LAG_U)
        def _():
            solve(i - LAG_U)

    for k in range(1, lev):
        take(wrecv.at[0], w_send.at[2, k])
    for up, cond, _, _ in edges:
        @pl.when(cond)
        def _():
            for h in range(halves):
                take(wrecv.at[0], w_send.at[up, h])
    whole = state0.at[0, :, pl.ds(0, rows)]
    for k in range(1, span * halves):
        take(whole, in_send.at[k])
        take(whole, out_send.at[k])

    def drain(up, at):
        _, count, _ = reach(at, up)
        if count > 0:
            for h in range(halves):
                take(state0.at[0, :, pl.ds(0, count)], d_send.at[up, h])
        total = sum(reach(other, up)[1] for other in range(span) if other != at)
        if total > 0:
            take(state0.at[:, :, pl.ds(0, total)], r_send.at[up])

    each_way(drain)
    for up, cond in ((1, has_up), (0, has_down)):
        pl.when(cond)(functools.partial(take, state2.at[:, :, pl.ds(0, PAD)], b_send.at[up]))

    others = stats.at[pl.ds(0, n - 1)]
    take(others, s_send)
    take(others, s_recv)
    total = stats[0]
    for k in range(1, n):
        total = total + stats[k]
    line = jnp.broadcast_to(total[0:1] / total[1:2], (SUB, LANES))
    quotient = line
    for k in range(1, SUB):
        quotient = jnp.where(sub == k, pltpu.roll(line, LANES - k * SLOT, 1), quotient)
    for c in range(chunks * groups):
        scal[pl.ds(c * SUB, SUB), :] = jnp.broadcast_to(quotient[:, c:c + 1], (SUB, LANES))

    def mixed(s, scale, o):
        at = pl.ds(s * lev * rows + o * SUB, SUB)
        return scale * flat_b[at, :] + out_ref[at, :]

    m0 = [mixed(0, scal[0:1, :], o) for o in range(pairs)]
    above = zero
    fades = [None] * pairs
    for o in range(pairs - 1, -1, -1):
        turn = flip(m0[o])
        col = above + 0.5 * m0[o] + jnp.where(low, turn, 0.0)
        fades[o] = jnp.exp((-0.5 / lev) * col)
        above = above + (m0[o] + turn)

    @pl.loop(0, chunks)
    def _(c):
        for i in range(chunk):
            s = c * chunk + i
            scale = scal[pl.ds(c * groups * SUB + i, 1), :]
            rate = rate_ref[s]
            for o in range(pairs):
                out_ref[pl.ds(s * lev * rows + o * SUB, SUB), :] = (
                    mixed(s, scale, o) * jnp.exp(-(rate * fades[o])))


def per_device(gx_n, halves, conc, winds, diffusivity, emission, photo_rate):
    spec, lev, rows, lanes = conc.shape
    span = lev // halves
    assert span * halves == lev and gx_n % span == 0 and lev % 2 == 0
    assert lanes == LANES and 2 * rows == SUB and span * rows == SUB and spec % 2 == 0
    n = gx_n * halves
    chunk = max(d for d in range(1, WIDTH + 1) if spec % d == 0)
    chunks = spec // chunk
    groups = -(-chunk // SUB)
    assert chunks * groups <= SLOT and gx_n // span <= chunks + LAG_B
    deep = span * rows
    dims = (spec, lev, rows, halves, gx_n, span, chunk)
    f32 = jnp.float32
    hbm = pl.BlockSpec(memory_space=pl.ANY)
    dma = pltpu.SemaphoreType.DMA
    slots = (span + 2) * halves
    out = pl.pallas_call(
        functools.partial(kernel, dims),
        out_shape=pltpu.VMEM((spec * lev * rows, lanes), f32),
        in_specs=[hbm] * 5,
        out_specs=pl.BlockSpec(memory_space=pltpu.VMEM),
        scratch_shapes=[
            pltpu.SMEM((spec,), f32),
            pltpu.VMEM((lev - 1, rows, lanes), f32),
            pltpu.VMEM((spec * rows, lanes), f32),
            pltpu.VMEM((halves, spec, deep + 2 * SUB, lanes), f32),
            pltpu.VMEM((halves, chunk, 2 * SUB, lanes), f32),
            pltpu.VMEM((halves, spec, 2 * SUB, lanes), f32),
            pltpu.VMEM((halves, spec, deep, lanes), f32),
            pltpu.VMEM((spec, lev, rows, lanes), f32),
            pltpu.VMEM((slots, 2, rows, lanes), f32),
            pltpu.VMEM((2, halves, deep + 2 * SUB, lanes), f32),
            pltpu.VMEM((4, halves, 14, SUB, lanes), f32),
            pltpu.VMEM((2, groups * SUB * SUB, lanes), f32),
            pltpu.VMEM((SUB, lanes), f32),
            pltpu.VMEM((2, lanes), f32),
            pltpu.VMEM((n, 2, lanes), f32),
            pltpu.VMEM((chunks * groups * SUB, lanes), f32),
            dma((3,)),
            dma((3, lev)), dma((slots,)),
            dma((lev,)), dma((span, chunks)), dma(()),
            dma((2, halves)), dma((2,)), dma((2,)), dma((2, chunks)),
            dma((2,)), dma((2, chunks)),
            dma((lev,)), dma((chunks,)),
            dma(()), dma(()), pltpu.SemaphoreType.REGULAR((2,)),
        ],
        compiler_params=pltpu.CompilerParams(collective_id=0, has_side_effects=True),
    )(
        conc,
        winds,
        diffusivity,
        emission.reshape(spec * rows, lanes),
        photo_rate,
    )
    return out.reshape(spec, lev, rows, lanes)


def solution(mesh):
    halves = mesh.shape["gy"]
    gx_n = mesh.shape["gx"]
    return jax.shard_map(
        functools.partial(per_device, gx_n, halves),
        mesh=mesh,
        in_specs=(
            P(None, None, ("member", "gx"), "gy"),
            P(None, None, ("member", "gx"), "gy"),
            P(None, ("member", "gx"), "gy"),
            P(None, ("member", "gx"), "gy"),
            P(),
        ),
        out_specs=P(None, None, ("member", "gx"), "gy"),
        check_vma=False,
    )
```

```python
import functools

import jax
import jax.numpy as jnp
from jax import lax
from jax.experimental import pallas as pl
from jax.experimental.pallas import tpu as pltpu
from jax.sharding import PartitionSpec as P

BETAS = (1.0 / 3.0, 0.5, 1.0)
SUB = 8
LANES = 128
PAD = 3
WIDE = 2 * PAD
LAG_A = 6
LAG_B = 11
LAG_U = 16
WIDTH = 11
SLOT = LANES // SUB
MESH = pl.DeviceIdType.MESH


def stencil_weights(km, kp):
    def face(k):
        k = k / 60.0
        a = jnp.abs(k)
        return (
            k + a,
            -8.0 * k - 5.0 * a,
            37.0 * k + 10.0 * a,
            37.0 * k - 10.0 * a,
            -8.0 * k + 5.0 * a,
            k - a,
        )

    m, p = face(km), face(kp)
    return [-m[0]] + [p[j] - m[j + 1] for j in range(5)] + [p[5]]


def kernel(dims, conc_hbm, wind_hbm, diff_hbm, emis_hbm, rate_hbm, out_ref,
           rate_ref, diff_ref, emis_ref, state0, state1, state2, result, back,
           wrecv, cbuf, wts, part, stat, note, stats, scal,
           load_sem, w_send, w_recv, in_send, in_recv, own_recv, d_send, d_recv, r_send, a_recv,
           b_send, b_recv, out_send, out_recv, s_send, s_recv, token):
    spec, lev, rows, halves, gx_n, span, chunk = dims
    n = gx_n * halves
    chunks = spec // chunk
    groups = -(-chunk // SUB)
    deep = span * rows
    crews = gx_n // span
    slab, slab1, slab2 = deep + 2 * SUB, 2 * SUB, 2 * SUB
    my_gx, my_gy = lax.axis_index("gx"), lax.axis_index("gy")
    me = my_gx * halves + my_gy
    crew, seat = my_gx // span, my_gx % span
    my_lev = seat * halves + my_gy
    has_down, has_up = crew > 0, crew < crews - 1
    here = my_gx, my_gy

    def where_is(dev):
        return {"gx": dev[0], "gy": dev[1]}

    def beyond(dev, up):
        return dev[0] + (span if up else -span), dev[1]

    def mate(at, half):
        return crew * span + at, half

    barrier = pltpu.get_barrier_semaphore()

    def greet(dev):
        pl.semaphore_signal(barrier, inc=1, device_id=where_is(dev), device_id_type=MESH)

    peers = [((seat + k) % span, h) for k in range(1, span) for h in range(halves)]
    peers += [(seat, (my_gy + k) % halves) for k in range(1, halves)]
    for at, h in peers:
        greet(mate(at, h))
    for cond, up in ((has_up, 1), (has_down, 0)):
        @pl.when(cond)
        def _():
            for h in range(halves):
                greet(beyond(mate(seat, h), up))

    loads = [pltpu.make_async_copy(src, dst, load_sem.at[i]) for i, (src, dst) in enumerate(
        ((diff_hbm, diff_ref), (emis_hbm, emis_ref), (rate_hbm, rate_ref)))]
    for load in loads:
        load.start()

    def push(src, dst, dev, s_sem, r_sem):
        pltpu.make_async_remote_copy(
            src_ref=src, dst_ref=dst, send_sem=s_sem, recv_sem=r_sem,
            device_id=where_is(dev), device_id_type=MESH).start()

    def local(src, dst, r_sem):
        pltpu.make_async_copy(src, dst, r_sem).start()

    def take(like, sem):
        pltpu.make_async_copy(like, like, sem).wait()

    def group(c):
        return pl.ds(c * chunk, chunk)

    flat0 = state0.reshape(halves * spec * slab, LANES)
    flat1 = state1.reshape(halves * chunk * slab1, LANES)
    flat2 = state2.reshape(halves * spec * slab2, LANES)
    flat_r = result.reshape(halves * spec * deep, LANES)
    flat_b = back.reshape(spec * lev * rows, LANES)
    zero = jnp.zeros((SUB, LANES), jnp.float32)
    few = jnp.zeros((SUB // 2, LANES), jnp.float32)

    pl.semaphore_wait(barrier, lev - 1 + jnp.where(has_down, halves, 0) + jnp.where(has_up, halves, 0))

    own_rows = pl.ds(SUB + seat * rows, rows)

    def send_in(c):
        dst = state0.at[my_gy, group(c), own_rows]
        for k in range(1, span):
            at = (seat + k) % span
            for h in range(halves):
                push(conc_hbm.at[group(c), at * halves + h], dst, mate(at, h),
                     in_send.at[k * halves + h], in_recv.at[seat, c])

    def send_own():
        dst = state0.at[my_gy, :, own_rows]
        for k in range(1, halves):
            h = (my_gy + k) % halves
            push(conc_hbm.at[:, seat * halves + h], dst, mate(seat, h), in_send.at[k], own_recv)
        local(conc_hbm.at[:, my_lev], dst, own_recv)

    def reach(at, up):
        if up:
            first = max(0, deep - WIDE - at * rows)
            return first, rows - first, SUB - deep + at * rows + first
        return 0, max(0, min(rows, WIDE - at * rows)), SUB + deep + at * rows

    def each_way(act, landing=False):
        for up, cond in ((0, has_up if landing else has_down), (1, has_down if landing else has_up)):
            for at in range(span):
                pl.when(cond & (seat == at))(functools.partial(act, up, at))

    def send_direct():
        def act(up, at):
            first, count, land = reach(at, up)
            if count > 0:
                for h in range(halves):
                    push(conc_hbm.at[:, at * halves + h, pl.ds(first, count)],
                         state0.at[my_gy, :, pl.ds(land, count)],
                         beyond(mate(at, h), up),
                         d_send.at[up, h], d_recv.at[up])

        each_way(act)

    def send_relay(c):
        def act(up, at):
            for other in range(span):
                first, count, land = reach(other, up)
                if other != at and count > 0:
                    push(state0.at[:, group(c), pl.ds(SUB + other * rows + first, count)],
                         state0.at[:, group(c), pl.ds(land, count)],
                         beyond(here, up), r_send.at[up], a_recv.at[up, c])

        each_way(act)

    edges = ((1, has_up, span - 1, 0), (0, has_down, 0, span + 1))

    def send_winds():
        for k, (at, h) in enumerate(peers):
            push(wind_hbm.at[:, at * halves + h], wrecv.at[(seat + 1) * halves + my_gy], mate(at, h),
                 w_send.at[2, k + 1], w_recv.at[(seat + 1) * halves + my_gy])
        local(wind_hbm.at[:, my_lev], wrecv.at[(seat + 1) * halves + my_gy],
              w_recv.at[(seat + 1) * halves + my_gy])
        for up, cond, edge, slot in edges:
            @pl.when(cond & (seat == edge))
            def _():
                for h in range(halves):
                    push(wind_hbm.at[:, edge * halves + h], wrecv.at[slot * halves + my_gy],
                         beyond(mate(edge, h), up),
                         w_send.at[up, h], w_recv.at[slot * halves + my_gy])

    def relay_winds():
        for at in range(span):
            for h in range(halves):
                k = (at + 1) * halves + h
                take(wrecv.at[k], w_recv.at[k])
        for up, cond, edge, slot in edges:
            @pl.when(cond & (seat != edge))
            def _():
                for h in range(halves):
                    push(wrecv.at[(edge + 1) * halves + h], wrecv.at[slot * halves + h],
                         beyond(here, up),
                         w_send.at[up, h], w_recv.at[slot * halves + h])

    send_winds()
    send_in(0)
    send_direct()
    send_own()

    @pl.loop(1, chunks)
    def _(c):
        send_in(c)

    def clear(first0, first2):
        @pl.loop(0, halves * chunks)
        def _(i):
            for k in range(chunk):
                flat0[pl.ds((i * chunk + k) * slab + first0, SUB), :] = zero
                flat2[pl.ds((i * chunk + k) * slab2 + first2, SUB // 2), :] = few

    pl.when(crew == 0)(lambda: clear(0, 0))
    pl.when(crew == crews - 1)(lambda: clear(SUB + deep, SUB // 2 + deep))
    for h in range(halves):
        for c in range(2):
            cbuf[c, h, 0:SUB, :] = zero
            cbuf[c, h, SUB + deep:2 * SUB + deep, :] = zero
    part[...] = jnp.zeros_like(part)
    stat[...] = zero

    lane = lax.broadcasted_iota(jnp.int32, (SUB, LANES), 1)
    sub = lax.broadcasted_iota(jnp.int32, (SUB, LANES), 0)

    for load in loads:
        load.wait()
    ks = [diff_ref[lv] for lv in range(lev - 1)]
    none = jnp.zeros((rows, LANES), jnp.float32)
    lower, upper = [none] + ks, ks + [none]
    inv, ratio = [], []
    for lv in range(lev):
        pivot = 1.0 + lower[lv] + upper[lv]
        if lv:
            pivot = pivot - lower[lv] * ratio[-1]
        inv.append(1.0 / pivot)
        ratio.append(upper[lv] * inv[lv])
    inverse = [[None] * lev for _ in range(lev)]
    for j in range(lev):
        val = [none] * lev
        for lv in range(j, lev):
            val[lv] = inv[lv] if lv == j else lower[lv] * val[lv - 1] * inv[lv]
        for lv in range(lev - 1, -1, -1):
            inverse[lv][j] = val[lv] if lv == lev - 1 else val[lv] + ratio[lv] * inverse[lv + 1][j]
    pairs = lev // 2

    def duo(a, b):
        return jnp.concatenate([a, b], axis=0)

    mats = [[(duo(inverse[2 * o][2 * i], inverse[2 * o + 1][2 * i + 1]),
              duo(inverse[2 * o][2 * i + 1], inverse[2 * o + 1][2 * i]))
             for i in range(pairs)] for o in range(pairs)]
    first_col = [duo(inverse[2 * o][0], inverse[2 * o + 1][0]) for o in range(pairs)]

    def flip(v):
        return pltpu.roll(v, SUB // 2, 0)

    low = sub < SUB // 2

    @pl.loop(0, spec // 2)
    def _(s):
        e = emis_ref[pl.ds(s * SUB, SUB), :]
        f = flip(e)
        for k, v in enumerate((jnp.where(low, e, f), jnp.where(low, f, e))):
            for o in range(pairs):
                out_ref[pl.ds((2 * s + k) * lev * rows + o * SUB, SUB), :] = first_col[o] * v

    relay_winds()

    passes = ((0, -PAD), (0, deep - SUB + PAD), (1, 0), (2, 0))

    def weigh():
        def wind_in(slot, wait=True):
            for h in range(halves):
                if wait:
                    take(wrecv.at[slot * halves + h], w_recv.at[slot * halves + h])
                for c in range(2):
                    base = SUB + (slot - 1) * rows
                    cbuf[c, h, base:base + rows, :] = wrecv[slot * halves + h, c]

        for slot in range(1, span + 1):
            wind_in(slot, False)
        pl.when(has_down)(lambda: wind_in(0))
        pl.when(has_up)(lambda: wind_in(span + 1))

        for q, (s, r0) in enumerate(passes):
            at_row = crew * deep + r0 + sub
            inside = (at_row >= 0) & (at_row < crews * deep)
            for h in range(halves):
                here, left, right = (cbuf[0, h, SUB + r0 + d:2 * SUB + r0 + d, :] for d in (0, -1, 1))
                for j, w in enumerate(stencil_weights(0.5 * (left + here), 0.5 * (here + right))):
                    wts[q, h, j] = jnp.where(inside, w, 0.0) * BETAS[s]
            cy = [cbuf[1, h, SUB + r0:2 * SUB + r0, :] for h in range(halves)]
            for h in range(halves):
                nxt = pltpu.roll(cy[h + 1], LANES - 1, 1) if h + 1 < halves else zero
                prv = pltpu.roll(cy[h - 1], 1, 1) if h > 0 else zero
                up = jnp.where(lane < LANES - 1, pltpu.roll(cy[h], LANES - 1, 1), nxt)
                down = jnp.where(lane >= 1, pltpu.roll(cy[h], 1, 1), prv)
                ws = stencil_weights(0.5 * (down + cy[h]), 0.5 * (cy[h] + up))
                for j, w in enumerate(ws):
                    d = j - 3
                    if d > 0 and h == halves - 1:
                        w = jnp.where(lane < LANES - d, w, 0.0)
                    if d < 0 and h == 0:
                        w = jnp.where(lane >= -d, w, 0.0)
                    wts[q, h, 7 + j] = w * BETAS[s]

    def step(q, count, src, src_at, start, start_at, put):
        wx = [[wts[q, h, j] for j in range(7)] for h in range(halves)]
        wy = [[wts[q, h, 7 + j] for j in range(7)] for h in range(halves)]
        for i in range(count):
            partial, new = [], []
            for h in range(halves):
                base = src_at(h, i)
                mid = None
                acc = None
                for j in range(7):
                    v = src[pl.ds(base + j, SUB), :]
                    if j == PAD:
                        mid = v
                    acc = wx[h][j] * v if acc is None else acc + wx[h][j] * v
                p = mid - acc
                partial.append(p)
                begin = mid if start is None else start[pl.ds(start_at(h, i), SUB), :]
                new.append(begin - acc - wy[h][3] * p)
            for d in (1, 2, 3):
                up = [pltpu.roll(p, LANES - d, 1) for p in partial]
                down = [pltpu.roll(p, d, 1) for p in partial]
                for h in range(halves):
                    u = up[h] if h == halves - 1 else jnp.where(lane < LANES - d, up[h], up[h + 1])
                    w = down[h] if h == 0 else jnp.where(lane >= d, down[h], down[h - 1])
                    new[h] = new[h] - (wy[h][3 + d] * u + wy[h][3 - d] * w)
            put(i, new)

    def at0(c):
        return lambda h, i: (h * spec + c * chunk + i) * slab

    def send_edge(c):
        for up, cond in ((1, has_up), (0, has_down)):
            first = SUB // 2 + (deep - PAD if up else 0)
            land = SUB // 2 + (-PAD if up else deep)
            pl.when(cond)(functools.partial(
                push, state2.at[:, group(c), pl.ds(first, PAD)],
                state2.at[:, group(c), pl.ds(land, PAD)],
                beyond(here, up), b_send.at[up], b_recv.at[up, c]))

    def arrive(up, at):
        count = reach(at, up)[1]
        if count > 0:
            take(state0.at[:, :, pl.ds(0, count)], d_recv.at[up])

    def arrive_relay(c, up, at):
        total = sum(reach(other, up)[1] for other in range(span) if other != at)
        if total > 0:
            take(state0.at[:, group(c), pl.ds(0, total)], a_recv.at[up, c])

    def early(c):

        @pl.when(c == 0)
        def _():
            take(state0.at[:, :, pl.ds(0, rows)], own_recv)
            each_way(arrive, True)

        each_way(functools.partial(arrive_relay, c), True)
        base = at0(c)
        for q in (0, 1):
            off = passes[q][1]

            def put(i, new, off=off):
                for h in range(halves):
                    flat1[pl.ds((h * chunk + i) * slab1 + off + PAD, SUB), :] = new[h]

            step(q, chunk, flat0, lambda h, i: base(h, i) + SUB + off - PAD, None, None, put)

        def put(i, new):
            for h in range(halves):
                flat2[pl.ds((h * spec + c * chunk + i) * slab2 + SUB // 2, SUB), :] = new[h]

        step(2, chunk, flat1, lambda h, i: (h * chunk + i) * slab1, flat0,
             lambda h, i: base(h, i) + SUB, put)
        send_edge(c)

    def late(c):
        pl.when(has_down)(lambda: take(state2.at[:, group(c), pl.ds(0, PAD)], b_recv.at[1, c]))
        pl.when(has_up)(lambda: take(state2.at[:, group(c), pl.ds(0, PAD)], b_recv.at[0, c]))
        base = at0(c)

        def put(i, new):
            net, pos = None, None
            for h in range(halves):
                flat_r[pl.ds((h * spec + c * chunk + i) * deep, SUB), :] = new[h]
                p = jnp.maximum(new[h], 0.0)
                net, pos = (new[h], p) if net is None else (net + new[h], pos + p)
            part[0, pl.ds(i * SUB, SUB), :] = net
            part[1, pl.ds(i * SUB, SUB), :] = pos

        step(3, chunk, flat2, lambda h, i: (h * spec + c * chunk + i) * slab2 + SUB // 2 - PAD,
             flat0, lambda h, i: base(h, i) + SUB, put)
        acc = stat[...]
        for o in range(2):
            for g in range(groups):
                first = g * SUB * SUB
                tot = part[o, pl.ds(first, SUB, stride=SUB), :]
                for r in range(1, SUB):
                    tot = tot + part[o, pl.ds(first + r, SUB, stride=SUB), :]
                acc = jnp.where(lane == c * groups + g + o * (LANES // 2),
                                jnp.sum(tot, axis=1, keepdims=True), acc)
        stat[...] = acc

        @pl.when(c == chunks - 1)
        def _():
            def send_stat(k, carry):
                dev = k - 1 + jnp.where(k - 1 >= me, 1, 0)
                dev = dev // halves, dev % halves
                push(note, stats.at[me], dev, s_send, s_recv)
                return carry

            rows_of = []
            for o in range(2):
                mine = jnp.where(lane < SLOT, pltpu.roll(acc, o * (LANES // 2), 1), 0.0)
                spread = pltpu.roll(mine, 0, 1, stride=SLOT, stride_axis=0)
                rows_of.append(jnp.sum(spread, axis=0, keepdims=True))
            packed = jnp.concatenate(rows_of, axis=0)
            note[...] = packed
            lax.fori_loop(1, n, send_stat, 0)
            stats[pl.ds(me, 1)] = packed[None]

        for k, (at, h) in enumerate(peers):
            push(result.at[h, group(c), pl.ds(at * rows, rows)],
                 back.at[group(c), my_lev], mate(at, h), out_send.at[k + 1], out_recv.at[c])
        local(result.at[my_gy, group(c), pl.ds(seat * rows, rows)],
              back.at[group(c), my_lev], out_recv.at[c])

    def solve(c):
        take(back.at[group(c)], out_recv.at[c])
        for i in range(chunk):
            base = (c * chunk + i) * lev * rows
            tiles = [jnp.maximum(flat_b[pl.ds(base + o * SUB, SUB), :], 0.0) for o in range(pairs)]
            swaps = [flip(t) for t in tiles]
            for o in range(pairs):
                acc = None
                for k in range(pairs):
                    term = mats[o][k][0] * tiles[k] + mats[o][k][1] * swaps[k]
                    acc = term if acc is None else acc + term
                flat_b[pl.ds(base + o * SUB, SUB), :] = acc

    def pass_on(up):
        pl.semaphore_signal(token.at[up], inc=1, device_id=where_is(beyond(here, up)),
                            device_id_type=MESH)

    pl.when(has_up & (crew == 0))(lambda: pass_on(1))
    pl.when(has_down & (crew == crews - 1))(lambda: pass_on(0))

    @pl.loop(0, chunks + LAG_U)
    def _(i):
        for up, cond, on, turn in ((1, has_down, has_up, crew), (0, has_up, has_down, crews - 1 - crew)):
            @pl.when(cond & (i == turn))
            def _():
                pl.semaphore_wait(token.at[up], 1)
                pl.when(on)(functools.partial(pass_on, up))

        @pl.when(i < chunks)
        def _():
            for k in range(1, span):
                at = (seat + k) % span
                take(state0.at[:, group(i), pl.ds(0, rows)], in_recv.at[at, i])
            send_relay(i)

        pl.when(i == LAG_A)(weigh)

        @pl.when((i >= LAG_A) & (i < LAG_A + chunks))
        def _():
            early(i - LAG_A)

        @pl.when((i >= LAG_B) & (i < LAG_B + chunks))
        def _():
            late(i - LAG_B)

        @pl.when(i >= LAG_U)
        def _():
            solve(i - LAG_U)

    for k in range(1, lev):
        take(wrecv.at[0], w_send.at[2, k])
    for up, cond, _, _ in edges:
        @pl.when(cond)
        def _():
            for h in range(halves):
                take(wrecv.at[0], w_send.at[up, h])
    whole = state0.at[0, :, pl.ds(0, rows)]
    for k in range(1, span * halves):
        take(whole, in_send.at[k])
        take(whole, out_send.at[k])

    def drain(up, at):
        _, count, _ = reach(at, up)
        if count > 0:
            for h in range(halves):
                take(state0.at[0, :, pl.ds(0, count)], d_send.at[up, h])
        total = sum(reach(other, up)[1] for other in range(span) if other != at)
        if total > 0:
            take(state0.at[:, :, pl.ds(0, total)], r_send.at[up])

    each_way(drain)
    for up, cond in ((1, has_up), (0, has_down)):
        pl.when(cond)(functools.partial(take, state2.at[:, :, pl.ds(0, PAD)], b_send.at[up]))

    others = stats.at[pl.ds(0, n - 1)]
    take(others, s_send)
    take(others, s_recv)
    total = stats[0]
    for k in range(1, n):
        total = total + stats[k]
    line = jnp.broadcast_to(total[0:1] / total[1:2], (SUB, LANES))
    quotient = line
    for k in range(1, SUB):
        quotient = jnp.where(sub == k, pltpu.roll(line, LANES - k * SLOT, 1), quotient)
    for c in range(chunks * groups):
        scal[pl.ds(c * SUB, SUB), :] = jnp.broadcast_to(quotient[:, c:c + 1], (SUB, LANES))

    def mixed(s, scale, o):
        at = pl.ds(s * lev * rows + o * SUB, SUB)
        return scale * flat_b[at, :] + out_ref[at, :]

    m0 = [mixed(0, scal[0:1, :], o) for o in range(pairs)]
    above = zero
    fades = [None] * pairs
    for o in range(pairs - 1, -1, -1):
        turn = flip(m0[o])
        col = above + 0.5 * m0[o] + jnp.where(low, turn, 0.0)
        fades[o] = jnp.exp((-0.5 / lev) * col)
        above = above + (m0[o] + turn)

    @pl.loop(0, chunks)
    def _(c):
        for i in range(chunk):
            s = c * chunk + i
            scale = scal[pl.ds(c * groups * SUB + i, 1), :]
            rate = rate_ref[s]
            for o in range(pairs):
                out_ref[pl.ds(s * lev * rows + o * SUB, SUB), :] = (
                    mixed(s, scale, o) * jnp.exp(-(rate * fades[o])))


def per_device(gx_n, halves, conc, winds, diffusivity, emission, photo_rate):
    spec, lev, rows, lanes = conc.shape
    span = lev // halves
    assert span * halves == lev and gx_n % span == 0 and lev % 2 == 0
    assert lanes == LANES and 2 * rows == SUB and span * rows == SUB and spec % 2 == 0
    n = gx_n * halves
    chunk = max(d for d in range(1, WIDTH + 1) if spec % d == 0)
    chunks = spec // chunk
    groups = -(-chunk // SUB)
    assert chunks * groups <= SLOT and gx_n // span <= chunks + LAG_B
    deep = span * rows
    dims = (spec, lev, rows, halves, gx_n, span, chunk)
    f32 = jnp.float32
    hbm = pl.BlockSpec(memory_space=pl.ANY)
    dma = pltpu.SemaphoreType.DMA
    slots = (span + 2) * halves
    out = pl.pallas_call(
        functools.partial(kernel, dims),
        out_shape=pltpu.VMEM((spec * lev * rows, lanes), f32),
        in_specs=[hbm] * 5,
        out_specs=pl.BlockSpec(memory_space=pltpu.VMEM),
        scratch_shapes=[
            pltpu.SMEM((spec,), f32),
            pltpu.VMEM((lev - 1, rows, lanes), f32),
            pltpu.VMEM((spec * rows, lanes), f32),
            pltpu.VMEM((halves, spec, deep + 2 * SUB, lanes), f32),
            pltpu.VMEM((halves, chunk, 2 * SUB, lanes), f32),
            pltpu.VMEM((halves, spec, 2 * SUB, lanes), f32),
            pltpu.VMEM((halves, spec, deep, lanes), f32),
            pltpu.VMEM((spec, lev, rows, lanes), f32),
            pltpu.VMEM((slots, 2, rows, lanes), f32),
            pltpu.VMEM((2, halves, deep + 2 * SUB, lanes), f32),
            pltpu.VMEM((4, halves, 14, SUB, lanes), f32),
            pltpu.VMEM((2, groups * SUB * SUB, lanes), f32),
            pltpu.VMEM((SUB, lanes), f32),
            pltpu.VMEM((2, lanes), f32),
            pltpu.VMEM((n, 2, lanes), f32),
            pltpu.VMEM((chunks * groups * SUB, lanes), f32),
            dma((3,)),
            dma((3, lev)), dma((slots,)),
            dma((lev,)), dma((span, chunks)), dma(()),
            dma((2, halves)), dma((2,)), dma((2,)), dma((2, chunks)),
            dma((2,)), dma((2, chunks)),
            dma((lev,)), dma((chunks,)),
            dma(()), dma(()), pltpu.SemaphoreType.REGULAR((2,)),
        ],
        compiler_params=pltpu.CompilerParams(collective_id=0, has_side_effects=True),
    )(
        conc,
        winds,
        diffusivity,
        emission.reshape(spec * rows, lanes),
        photo_rate,
    )
    return out.reshape(spec, lev, rows, lanes)


def solution(mesh):
    halves = mesh.shape["gy"]
    gx_n = mesh.shape["gx"]
    return jax.shard_map(
        functools.partial(per_device, gx_n, halves),
        mesh=mesh,
        in_specs=(
            P(None, None, ("member", "gx"), "gy"),
            P(None, None, ("member", "gx"), "gy"),
            P(None, ("member", "gx"), "gy"),
            P(None, ("member", "gx"), "gy"),
            P(),
        ),
        out_specs=P(None, None, ("member", "gx"), "gy"),
        check_vma=False,
    )
```
